128 devices in a mesh: col: 2 (over core), row: 64 (over z, y, x).
Axes of the slice: x: 4, y: 4, z: 4, core: 2. Of those that a mesh axis runs over, the one named last changes fastest.
Arguments:
- hyper_params: float32 [3], replicated
- w_in: float32 [16, 1024, 2816], P(None, 'row', 'col')
- x_in: bfloat16 [16, 1024, 1024], P(None, None, 'row')
- dy_in: bfloat16 [16, 1024, 2816], P(None, None, 'col')
- row_in: float32 [16, 1024], P(None, 'row')
- col_in: float32 [16, 2816], P(None, 'col')
- w_out: float32 [16, 2816, 1024], P(None, 'col', 'row')
- x_out: bfloat16 [16, 1024, 2816], P(None, None, 'col')
- dy_out: bfloat16 [16, 1024, 1024], P(None, None, 'row')
- row_out: float32 [16, 2816], P(None, 'col')
- col_out: float32 [16, 1024], P(None, 'row')
Outputs:
- output 1: float32 [16, 1024, 2816], P(None, 'row', 'col')
- output 2: float32 [16, 1024], P(None, 'row')
- output 3: float32 [16, 2816], P(None, 'col')
- output 4: float32 [16, 2816, 1024], P(None, 'col', 'row')
- output 5: float32 [16, 2816], P(None, 'col')
- output 6: float32 [16, 1024], P(None, 'row')
All inputs are finite; a program needn't handle non-finite values.
Results may differ from the reference program's by a relative error of at most 0.001.
Values are sent between devices in bfloat16 or wider.
A program may use at most 1 GiB of HBM per device.

```python
import jax
import jax.numpy as jnp
from jax import lax

LAYERS = 16
TOKENS = 1024
D_MODEL = 1024
D_FF = 2816
LATENT_RANK = 4
EPS_ONE = 1e-30
EPS_TWO = 1e-3
TWO_PI = 6.283185307179586


def profile(draw_key, length):
    phase_off = jax.random.uniform(draw_key, (LAYERS, LATENT_RANK, 1), jnp.float32) * TWO_PI
    freq_rank = (jnp.arange(LATENT_RANK) + 1).astype(jnp.float32)[None, :, None]
    position = (jnp.arange(length).astype(jnp.float32) / length)[None, None, :]
    return 1.0 + 0.9 * jnp.sin(TWO_PI * freq_rank * position + phase_off)


def draw_matrix(draw_key, n_rows, n_cols):
    sub_keys = jax.random.split(draw_key, 10)
    latent = jax.random.normal(sub_keys[0], (LAYERS, TOKENS, LATENT_RANK), jnp.float32)
    load_rows = jax.random.normal(sub_keys[1], (LAYERS, LATENT_RANK, n_rows), jnp.float32) * profile(sub_keys[2], n_rows)
    load_cols = jax.random.normal(sub_keys[3], (LAYERS, LATENT_RANK, n_cols), jnp.float32) * profile(sub_keys[4], n_cols)
    x_act = jnp.einsum('ltk,lkm->ltm', latent, load_rows) + jax.random.normal(sub_keys[5], (LAYERS, TOKENS, n_rows), jnp.float32)
    dy_act = (jnp.einsum('ltk,lkn->ltn', latent, load_cols) + jax.random.normal(sub_keys[6], (LAYERS, TOKENS, n_cols), jnp.float32)) / TOKENS
    w_mat = jax.random.normal(sub_keys[7], (LAYERS, n_rows, n_cols), jnp.float32) * n_rows ** -0.5
    row_stat = 6.0 * jnp.exp(0.5 * jax.random.normal(sub_keys[8], (LAYERS, n_rows), jnp.float32))
    col_stat = 6.0 * jnp.exp(0.5 * jax.random.normal(sub_keys[9], (LAYERS, n_cols), jnp.float32))
    return w_mat, x_act.astype(jnp.bfloat16), dy_act.astype(jnp.bfloat16), row_stat, col_stat


def setup_inputs(seed: int = 0) -> dict:
    sub_keys = jax.random.split(jax.random.key(seed), 3)
    low_end = jnp.array([0.5, 0.5, 0.2], dtype=jnp.float32)
    span_width = jnp.array([0.3, 0.5, 0.2], dtype=jnp.float32)
    hyper_params = low_end + span_width * jax.random.uniform(sub_keys[0], (3,), jnp.float32)
    w_in, x_in, dy_in, row_in, col_in = draw_matrix(sub_keys[1], D_MODEL, D_FF)
    w_out, x_out, dy_out, row_out, col_out = draw_matrix(sub_keys[2], D_FF, D_MODEL)
    return {'hyper_params': hyper_params, 'w_in': w_in, 'x_in': x_in, 'dy_in': dy_in, 'row_in': row_in, 'col_in': col_in, 'w_out': w_out, 'x_out': x_out, 'dy_out': dy_out, 'row_out': row_out, 'col_out': col_out}


def adafactor_one(w_mat, x_act, dy_act, row_old, col_old, hyper_params):
    beta_two = hyper_params[0]
    rho_step = hyper_params[1]
    clip_max = hyper_params[2]
    grad_mat = jnp.dot(x_act.T, dy_act, preferred_element_type=jnp.float32)
    sq_grad = grad_mat * grad_mat + EPS_ONE
    row_new = beta_two * row_old + (1.0 - beta_two) * jnp.mean(sq_grad, axis=1)
    col_new = beta_two * col_old + (1.0 - beta_two) * jnp.mean(sq_grad, axis=0)
    row_mean = jnp.mean(row_new)
    update = grad_mat * lax.rsqrt((row_new / row_mean)[:, None] * col_new[None, :])
    upd_rms = jnp.sqrt(jnp.mean(update * update))
    w_rms = jnp.sqrt(jnp.mean(w_mat * w_mat))
    step_size = rho_step * jnp.maximum(EPS_TWO, w_rms) / jnp.maximum(1.0, upd_rms / clip_max)
    return w_mat - step_size * update, row_new, col_new


def reference(hyper_params, w_in, x_in, dy_in, row_in, col_in, w_out, x_out, dy_out, row_out, col_out):
    def one_layer(layer_args):
        w_first, x_first, dy_first, row_first, col_first, w_second, x_second, dy_second, row_second, col_second = layer_args
        in_result = adafactor_one(w_first, x_first, dy_first, row_first, col_first, hyper_params)
        out_result = adafactor_one(w_second, x_second, dy_second, row_second, col_second, hyper_params)
        return in_result + out_result
    results = lax.map(one_layer, (w_in, x_in, dy_in, row_in, col_in, w_out, x_out, dy_out, row_out, col_out))
    return (results[0], results[1], results[2], results[3], results[4], results[5])
```

```python
import functools

import jax
import jax.numpy as jnp
from jax import lax
from jax.experimental import pallas as pl
from jax.experimental.pallas import tpu as pltpu
from jax.sharding import PartitionSpec as P

EPS_ONE = 1e-30
EPS_TWO = 1e-3
MESH = pl.DeviceIdType.MESH
LANES = 128
SLOTS = 10
LAG = 2


def torus_dims(n_row):
    side = round(n_row ** (1.0 / 3.0))
    return side, side, side


def kernel(dims, hyper, a_in, b_in, w_in, side_in, lane_in, a_out, b_out, w_out, lane_out, side_out,
           o_w_in, o_side_in, o_lane_in, o_w_out, o_lane_out, o_side_out,
           hyper_s, a_v, b_v, g_v, w_v, side_old, lane_old, side_res, lane_res, old_pack, side_new,
           fac_v, new_pack, row_buf, aux_buf, x_buf, y_buf, z_buf, acc_v, fx_buf, fy_buf, fz_buf,
           load_sem, b_sem, store_sem, send_sem, x_sem, aux_sem, row_sem, y_sem, z_sem, f_sem):
    nz, ny, nx = dims
    layers, _, width = w_in.shape
    depth = a_in.shape[1]
    chunks = width // LANES
    n_row = nz * ny * nx
    n_side = float(depth * n_row)
    n_lane = float(width * 2)
    n_total = n_side * n_lane

    row = lax.axis_index("row")
    core = lax.axis_index("col")
    my_x = lax.rem(row, nx)
    my_y = lax.rem(row // nx, ny)
    my_z = row // (nx * ny)

    def dev(z, y, x, c):
        return {"row": (z * ny + y) * nx + x, "col": c}

    other = 1 - core
    x_peers = [lax.rem(my_x + d, nx) for d in range(1, nx)]
    y_peers = [lax.rem(my_y + d, ny) for d in range(1, ny)]
    z_peers = [lax.rem(my_z + d, nz) for d in range(1, nz)]
    x_devs = [dev(my_z, my_y, x, core) for x in x_peers]
    c_devs = [dev(my_z, my_y, x, other) for x in x_peers + [my_x]]
    y_devs = [dev(my_z, y, my_x, core) for y in y_peers]
    z_devs = [dev(z, my_y, my_x, core) for z in z_peers]
    partner = c_devs[-1]

    b_refs = (b_in, b_out)

    def b_copy(layer, j):
        slot = lax.rem(2 * layer + j, SLOTS)
        return pltpu.make_async_copy(b_refs[j].at[layer], b_v.at[slot], b_sem.at[slot])

    small = [(hyper, hyper_s), (a_in, a_v.at[0]), (a_out, a_v.at[1]), (side_in, side_old.at[0]), (side_out, side_old.at[1]),
             (lane_in, lane_old.at[0]), (lane_out, lane_old.at[1])]
    small = [pltpu.make_async_copy(s, d, load_sem.at[i]) for i, (s, d) in enumerate(small)]
    big = [pltpu.make_async_copy(s, w_v.at[j], load_sem.at[len(small) + j]) for j, s in enumerate((w_in, w_out))]
    for c in small:
        c.start()
    for s in range(SLOTS):
        b_copy(s // 2, s % 2).start()
        if s == 3:
            for c in big:
                c.start()

    barrier = pltpu.get_barrier_semaphore()
    peers = x_devs + c_devs + y_devs + z_devs
    for d in peers:
        pl.semaphore_signal(barrier, inc=1, device_id=d, device_id_type=MESH)
    for c in small:
        c.wait()
    acc_v[...] = jnp.zeros_like(acc_v)
    beta = hyper_s[0]
    keep = 1.0 - beta
    eye = lax.broadcasted_iota(jnp.int32, (depth, depth), 0) == lax.broadcasted_iota(jnp.int32, (depth, depth), 1)
    lane_id = lax.broadcasted_iota(jnp.int32, (1, LANES), 1)
    pack_rows = x_buf.shape[2]
    pack_id = lax.broadcasted_iota(jnp.int32, (pack_rows, LANES), 0)
    aux_row = pack_rows - 8

    for layer in range(layers):
        for j in range(2):
            for k in range(chunks):
                old_pack[layer, j * chunks + k:j * chunks + k + 1, :] = lane_old[j, layer:layer + 1, k * LANES:(k + 1) * LANES]
            line = jnp.broadcast_to(side_old[j, layer:layer + 1, :], (depth, depth))
            line = jnp.sum(jnp.where(eye, line, 0.0), axis=1, keepdims=True)
            side_new[layer, j * depth:(j + 1) * depth, :] = jnp.broadcast_to(line, (depth, LANES))
        old_pack[layer, 2 * chunks:, :] = jnp.ones((pack_rows - 2 * chunks, LANES), jnp.float32)
    pl.semaphore_wait(barrier, len(peers))

    def send(src, dst, recv, d, k):
        pltpu.make_async_remote_copy(src_ref=src, dst_ref=dst, send_sem=send_sem.at[k], recv_sem=recv, device_id=d, device_id_type=MESH).start()

    def arrived(ref, sem):
        pltpu.make_async_copy(ref, ref, sem).wait()

    def stage_a(layer):
        for j in range(2):
            b_copy(layer, j).wait()
            slot = lax.rem(2 * layer + j, SLOTS)
            grad = jnp.dot(a_v[j, layer], b_v[slot], preferred_element_type=jnp.float32)
            nxt = layer + SLOTS // 2

            @pl.when(nxt < layers)
            def _():
                b_copy(nxt, j).start()

            g_v[j, layer] = grad
            sq = grad * grad + EPS_ONE
            lane_part = jnp.sum(sq, axis=0, keepdims=True)
            side_part = sq[:, :LANES]
            total = lane_part[:, :LANES]
            for k in range(chunks):
                cols = slice(k * LANES, (k + 1) * LANES)
                if k:
                    side_part = side_part + sq[:, cols]
                    total = total + lane_part[:, cols]
                x_buf[layer, my_x, j * chunks + k:j * chunks + k + 1, :] = lane_part[:, cols]
            row_buf[layer, core, j * depth:(j + 1) * depth, :] = side_part
            mean_part = total * (keep / n_total)
            if j == 0:
                old = jnp.sum(side_new[layer, :depth, :], axis=0, keepdims=True)
                mean_part = mean_part + old * (0.5 * beta / (n_side * LANES))
            else:
                old = jnp.sum(jnp.where((pack_id >= chunks) & (pack_id < 2 * chunks), old_pack[layer], 0.0), axis=0, keepdims=True)
                mean_part = mean_part + old * (beta / (n_lane * n_row))
            x_buf[layer, my_x, 2 * chunks + j:2 * chunks + j + 1, :] = mean_part
        for d in x_devs:
            send(x_buf.at[layer, my_x], x_buf.at[layer, my_x], x_sem.at[layer], d, 0)
        send(row_buf.at[layer, core], row_buf.at[layer, core], row_sem.at[layer], partner, 1)
        for d in c_devs:
            send(x_buf.at[layer, my_x, pl.ds(aux_row, 8)], aux_buf.at[layer, my_x], aux_sem.at[layer], d, 2)

    def stage_x(layer):
        arrived(x_buf.at[layer, pl.ds(0, nx - 1)], x_sem.at[layer])
        arrived(aux_buf.at[layer], aux_sem.at[layer])
        tot = x_buf[layer, 0]
        aux = aux_buf[layer, 0]
        for s in range(1, nx):
            tot = tot + x_buf[layer, s]
            aux = aux + aux_buf[layer, s]
        y_buf[layer, my_y] = tot
        tail = tot[aux_row:, :]
        last = lax.broadcasted_iota(jnp.int32, (8, LANES), 0) >= 2 * chunks - aux_row
        y_buf[layer, my_y, aux_row:, :] = jnp.where(last, tail + aux, tail)
        for d in y_devs:
            send(y_buf.at[layer, my_y], y_buf.at[layer, my_y], y_sem.at[layer], d, 3)
        arrived(row_buf.at[layer, 0], row_sem.at[layer])
        side_sum = jnp.sum(row_buf[layer, 0] + row_buf[layer, 1], axis=1, keepdims=True)
        side_new[layer] = beta * side_new[layer] + side_sum * (keep / n_lane)

    def stage_y(layer):
        arrived(y_buf.at[layer, pl.ds(0, ny - 1)], y_sem.at[layer])
        tot = y_buf[layer, 0]
        for s in range(1, ny):
            tot = tot + y_buf[layer, s]
        z_buf[layer, my_z] = tot
        for d in z_devs:
            send(z_buf.at[layer, my_z], z_buf.at[layer, my_z], z_sem.at[layer], d, 4)

    def stage_z(layer):
        arrived(z_buf.at[layer, pl.ds(0, nz - 1)], z_sem.at[layer])
        tot = z_buf[layer, 0]
        for s in range(1, nz):
            tot = tot + z_buf[layer, s]
        new = beta * old_pack[layer] + tot * (keep / n_side)
        new_pack[layer] = new
        mean = [jnp.sum(tot[2 * chunks + j:2 * chunks + j + 1, :], axis=1, keepdims=True) for j in range(2)]
        fac_v[...] = lax.rsqrt(jnp.where(pack_id < chunks, new, new / mean[1]))
        for j in range(2):
            side = side_new[layer, j * depth:(j + 1) * depth, :]
            side = lax.rsqrt(side / mean[0] if j == 0 else side)
            u_sq = None
            w_sq = None
            for k in range(chunks):
                cols = slice(k * LANES, (k + 1) * LANES)
                line = slice(j * chunks + k, j * chunks + k + 1)
                upd = g_v[j, layer, :, cols] * side * fac_v[line, :]
                g_v[j, layer, :, cols] = upd
                wgt = w_v[j, layer, :, cols]
                u_sq = upd * upd if k == 0 else u_sq + upd * upd
                w_sq = wgt * wgt if k == 0 else w_sq + wgt * wgt
            for i, part in enumerate((u_sq, w_sq)):
                part = jnp.sum(jnp.sum(part, axis=0, keepdims=True), axis=1, keepdims=True)
                line = slice(2 * i + j, 2 * i + j + 1)
                acc_v[line, :] = acc_v[line, :] + jnp.where(lane_id == layer, part, 0.0)

    def step(i, carry):
        pl.when(i < layers)(lambda: stage_a(i))
        pl.when((i >= LAG) & (i < layers + LAG))(lambda: stage_x(i - LAG))
        pl.when((i >= 2 * LAG) & (i < layers + 2 * LAG))(lambda: stage_y(i - 2 * LAG))

        @pl.when(i == 3 * LAG)
        def _():
            for c in big:
                c.wait()

        pl.when(i >= 3 * LAG)(lambda: stage_z(i - 3 * LAG))
        return carry

    lax.fori_loop(0, layers + 3 * LAG, step, 0)

    stores = [(side_res.at[0], o_side_in), (side_res.at[1], o_side_out), (lane_res.at[0], o_lane_in), (lane_res.at[1], o_lane_out)]
    stores = [pltpu.make_async_copy(s, d, store_sem.at[i]) for i, (s, d) in enumerate(stores)]

    def total(buf):
        out = buf[0]
        for s in range(1, buf.shape[0]):
            out = out + buf[s]
        return out

    slot = core * nx + my_x
    fx_buf[slot] = acc_v[...]
    for d in x_devs + c_devs:
        send(fx_buf.at[slot], fx_buf.at[slot], f_sem.at[0], d, 5)
    for layer in range(layers):
        for j in range(2):
            for k in range(chunks):
                lane_res[j, layer:layer + 1, k * LANES:(k + 1) * LANES] = new_pack[layer, j * chunks + k:j * chunks + k + 1, :]
            line = side_new[layer, j * depth:(j + 1) * depth, :depth]
            side_res[j, layer:layer + 1, :] = jnp.sum(jnp.where(eye, line, 0.0), axis=0, keepdims=True)
    for c in stores:
        c.start()
    arrived(fx_buf.at[pl.ds(0, 2 * nx - 1)], f_sem.at[0])
    fy_buf[my_y] = total(fx_buf)
    for d in y_devs:
        send(fy_buf.at[my_y], fy_buf.at[my_y], f_sem.at[1], d, 6)
    arrived(fy_buf.at[pl.ds(0, ny - 1)], f_sem.at[1])
    fz_buf[my_z] = total(fy_buf)
    for d in z_devs:
        send(fz_buf.at[my_z], fz_buf.at[my_z], f_sem.at[2], d, 7)
    arrived(fz_buf.at[pl.ds(0, nz - 1)], f_sem.at[2])
    tot = total(fz_buf)
    rms = jnp.sqrt(tot / n_total)
    rho = hyper_s[1]
    clip = hyper_s[2]
    scale = rho * jnp.maximum(EPS_TWO, rms[2:4, :]) / jnp.maximum(1.0, rms[0:2, :] / clip)
    o_w = (o_w_in, o_w_out)

    def finish(layer, carry):
        for j in range(2):
            amount = jnp.sum(jnp.where(lane_id == layer, scale[j:j + 1, :], 0.0), axis=1, keepdims=True)
            w_v[j, layer] = w_v[j, layer] - amount * g_v[j, layer]
            pltpu.make_async_copy(w_v.at[j, layer], o_w[j].at[layer], store_sem.at[4 + j]).start()
        return carry

    lax.fori_loop(0, layers, finish, 0)

    def sent(ref, k):
        pltpu.make_async_copy(ref, ref, send_sem.at[k]).wait()

    sent(x_buf.at[:, pl.ds(0, nx - 1)], 0)
    sent(row_buf.at[:, 0], 1)
    sent(aux_buf, 2)
    sent(y_buf.at[:, pl.ds(0, ny - 1)], 3)
    sent(z_buf.at[:, pl.ds(0, nz - 1)], 4)
    sent(fx_buf.at[pl.ds(0, 2 * nx - 1)], 5)
    sent(fy_buf.at[pl.ds(0, ny - 1)], 6)
    sent(fz_buf.at[pl.ds(0, nz - 1)], 7)
    for c in stores:
        c.wait()
    for j in range(2):
        pltpu.make_async_copy(w_v.at[j], o_w[j], store_sem.at[4 + j]).wait()


def solution(mesh):
    dims = torus_dims(mesh.shape['row'])
    nz, ny, nx = dims
    tile_in = P(None, 'row', 'col')
    tile_out = P(None, 'col', 'row')
    lane_row = P(None, None, 'row')
    lane_col = P(None, None, 'col')
    vec_row = P(None, 'row')
    vec_col = P(None, 'col')

    def local_step(hyper_params, w_in, x_in, dy_in, row_in, col_in, w_out, x_out, dy_out, row_out, col_out):
        layers, depth, width = w_in.shape
        tokens = x_in.shape[1]
        chunks = width // LANES
        pack = -(-(2 * chunks + 2) // 8) * 8
        f32 = jnp.float32
        turn = lambda v: jnp.swapaxes(v, 1, 2)
        vm = pltpu.VMEM
        dma = pltpu.SemaphoreType.DMA
        scratch = [
            pltpu.SMEM((3,), f32), vm((2, layers, depth, tokens), jnp.bfloat16), vm((SLOTS, tokens, width), jnp.bfloat16),
            vm((2, layers, depth, width), f32), vm((2, layers, depth, width), f32),
            vm((2, layers, depth), f32), vm((2, layers, width), f32), vm((2, layers, depth), f32), vm((2, layers, width), f32),
            vm((layers, pack, LANES), f32), vm((layers, 2 * depth, LANES), f32), vm((pack, LANES), f32), vm((layers, pack, LANES), f32),
            vm((layers, 2, 2 * depth, LANES), f32), vm((layers, nx, 8, LANES), f32),
            vm((layers, nx, pack, LANES), f32), vm((layers, ny, pack, LANES), f32), vm((layers, nz, pack, LANES), f32),
            vm((8, LANES), f32), vm((2 * nx, 8, LANES), f32), vm((ny, 8, LANES), f32), vm((nz, 8, LANES), f32),
            dma((9,)), dma((SLOTS,)), dma((6,)), dma((8,)), dma((layers,)), dma((layers,)), dma((layers,)), dma((layers,)), dma((layers,)), dma((3,)),
        ]
        shape = lambda *s: jax.ShapeDtypeStruct(s, f32)
        res = pl.pallas_call(
            functools.partial(kernel, dims),
            out_shape=(shape(layers, depth, width), shape(layers, depth), shape(layers, width), shape(layers, depth, width), shape(layers, width), shape(layers, depth)),
            in_specs=[pl.BlockSpec(memory_space=pl.ANY)] * 11,
            out_specs=[pl.BlockSpec(memory_space=pl.ANY)] * 6,
            scratch_shapes=scratch,
            name="adafactor_step",
            compiler_params=pltpu.CompilerParams(collective_id=0, has_side_effects=True, vmem_limit_bytes=60 * 1024 * 1024),
        )(hyper_params, turn(x_in), dy_in, w_in, row_in, col_in, turn(dy_out), x_out, turn(w_out), row_out, col_out)
        return res[0], res[1], res[2], turn(res[3]), res[4], res[5]

    return jax.shard_map(local_step, mesh=mesh, in_specs=(P(), tile_in, lane_row, lane_col, vec_row, vec_col, tile_out, lane_col, lane_row, vec_col, vec_row), out_specs=(tile_in, vec_row, vec_col, tile_out, vec_col, vec_row), check_vma=False)
```

```python
import functools

import jax
import jax.numpy as jnp
from jax import lax
from jax.experimental import pallas as pl
from jax.experimental.pallas import tpu as pltpu
from jax.sharding import PartitionSpec as P

EPS_ONE = 1e-30
EPS_TWO = 1e-3
MESH = pl.DeviceIdType.MESH
LANES = 128
SLOTS = 8
LAG = 3
VMEM_LIMIT = 48 * 1024 * 1024


def torus_dims(n_row):
    side = round(n_row ** (1.0 / 3.0))
    return side, side, side


def kernel(dims, hyper, a_in, b_in, w_in, side_in, lane_in, a_out, b_out, w_out, lane_out, side_out,
           w_v, side_res, lane_res,
           hyper_s, a_v, b_v, g_v, side_old, lane_old, old_pack, side_new,
           fac_v, new_pack, u_v, pair_buf, x_buf, y_buf, z_buf, fin_buf,
           load_sem, b_sem, send_sem, pair_sem, x_sem, y_sem, z_sem, fin_sem):
    nz, ny, nx = dims
    layers, depth, width = w_in.shape
    chunks = width // LANES
    n_row = nz * ny * nx
    n_side = float(depth * n_row)
    n_lane = float(width * 2)
    n_total = n_side * n_lane
    half = u_v.shape[1]

    row = lax.axis_index("row")
    core = lax.axis_index("col")
    my_x = lax.rem(row, nx)
    my_y = lax.rem(row // nx, ny)
    my_z = row // (nx * ny)

    def dev(z, y, x, c):
        return {"row": (z * ny + y) * nx + x, "col": c}

    x_devs = [dev(my_z, my_y, lax.rem(my_x + d, nx), core) for d in range(1, nx)]
    y_devs = [dev(my_z, lax.rem(my_y + d, ny), my_x, core) for d in range(1, ny)]
    z_devs = [dev(lax.rem(my_z + d, nz), my_y, my_x, core) for d in range(1, nz)]
    partner = dev(my_z, my_y, my_x, 1 - core)

    b_refs = (b_in, b_out)

    def b_copy(layer, j):
        slot = lax.rem(2 * layer + j, SLOTS)
        return pltpu.make_async_copy(b_refs[j].at[layer], b_v.at[slot], b_sem.at[slot])

    small = [(hyper, hyper_s), (a_in, a_v.at[0]), (a_out, a_v.at[1]), (side_in, side_old.at[0]), (side_out, side_old.at[1]),
             (lane_in, lane_old.at[0]), (lane_out, lane_old.at[1])]
    small = [pltpu.make_async_copy(s, d, load_sem.at[i]) for i, (s, d) in enumerate(small)]
    big = [pltpu.make_async_copy(s, w_v.at[j], load_sem.at[len(small) + j]) for j, s in enumerate((w_in, w_out))]
    for c in small:
        c.start()
    for s in range(SLOTS):
        b_copy(s // 2, s % 2).start()
        if s == 3:
            for c in big:
                c.start()

    barrier = pltpu.get_barrier_semaphore()
    peers = x_devs + y_devs + z_devs + [partner]
    for d in peers:
        pl.semaphore_signal(barrier, inc=1, device_id=d, device_id_type=MESH)
    for c in small:
        c.wait()

    beta = hyper_s[0]
    keep = 1.0 - beta
    eye = lax.broadcasted_iota(jnp.int32, (depth, depth), 0) == lax.broadcasted_iota(jnp.int32, (depth, depth), 1)
    half_id = lax.broadcasted_iota(jnp.int32, (half, LANES), 0)
    first = half_id < chunks
    second = (half_id >= chunks) & (half_id < 2 * chunks)

    for layer in range(layers):
        for j in range(2):
            for k in range(chunks):
                old_pack[layer, j * chunks + k:j * chunks + k + 1, :] = lane_old[j, layer:layer + 1, k * LANES:(k + 1) * LANES]
            line = jnp.broadcast_to(side_old[j, layer:layer + 1, :], (depth, depth))
            line = jnp.sum(jnp.where(eye, line, 0.0), axis=1, keepdims=True)
            side_new[layer, j * depth:(j + 1) * depth, :] = jnp.broadcast_to(line, (depth, LANES))
        old_pack[layer, 2 * chunks:, :] = jnp.ones((half - 2 * chunks, LANES), jnp.float32)
        line = jnp.sum(jnp.where(second, old_pack[layer], 0.0), axis=0, keepdims=True)
        pair_buf[layer, core, 2 * depth:, :] = jnp.broadcast_to(line, (8, LANES))
    pl.semaphore_wait(barrier, len(peers))

    def send(ref, recv, d, k):
        pltpu.make_async_remote_copy(src_ref=ref, dst_ref=ref, send_sem=send_sem.at[k], recv_sem=recv, device_id=d, device_id_type=MESH).start()

    def arrived(ref, sem):
        pltpu.make_async_copy(ref, ref, sem).wait()

    def total(buf, layer, count):
        out = buf[layer, 0]
        for s in range(1, count):
            out = out + buf[layer, s]
        return out

    def stage_a(layer):
        for j in range(2):
            b_copy(layer, j).wait()
            slot = lax.rem(2 * layer + j, SLOTS)
            grad = jnp.dot(a_v[j, layer], b_v[slot], preferred_element_type=jnp.float32)
            nxt = layer + SLOTS // 2

            @pl.when(nxt < layers)
            def _():
                b_copy(nxt, j).start()

            g_v[j, layer] = grad
            sq = grad * grad + EPS_ONE
            lane_part = jnp.sum(sq, axis=0, keepdims=True)
            side_part = sq[:, :LANES]
            for k in range(chunks):
                cols = slice(k * LANES, (k + 1) * LANES)
                if k:
                    side_part = side_part + sq[:, cols]
                x_buf[layer, my_x, j * chunks + k:j * chunks + k + 1, :] = lane_part[:, cols]
            pair_buf[layer, core, j * depth:(j + 1) * depth, :] = side_part
        send(pair_buf.at[layer, core], pair_sem.at[layer], partner, 0)

    def stage_d(layer):
        arrived(pair_buf.at[layer, 0], pair_sem.at[layer])
        both = total(pair_buf, layer, 2)
        side_sum = jnp.sum(both[:2 * depth], axis=1, keepdims=True)
        new = beta * side_new[layer] + side_sum * (keep / n_lane)
        side_new[layer] = new
        inv = lax.rsqrt(new)
        for j in range(2):
            fac = inv[j * depth:(j + 1) * depth]
            w_sq = None
            for k in range(chunks):
                cols = slice(k * LANES, (k + 1) * LANES)
                upd = g_v[j, layer, :, cols] * fac
                g_v[j, layer, :, cols] = upd
                x_buf[layer, my_x, half + j * chunks + k:half + j * chunks + k + 1, :] = jnp.sum(upd * upd, axis=0, keepdims=True)
                wgt = w_v[j, layer, :, cols]
                w_sq = wgt * wgt if k == 0 else w_sq + wgt * wgt
            x_buf[layer, my_x, half + 2 * chunks + j:half + 2 * chunks + j + 1, :] = jnp.sum(w_sq, axis=0, keepdims=True)
        mean_in = jnp.sum(new[:depth], axis=0, keepdims=True) * (1.0 / (n_side * LANES))
        mean_out = jnp.broadcast_to(jnp.sum(side_sum[depth:], axis=0, keepdims=True), (1, LANES)) * (keep / (n_total * LANES))
        mean_out = mean_out + both[2 * depth:2 * depth + 1] * (beta / (n_lane * n_row))
        x_buf[layer, my_x, 2 * chunks:2 * chunks + 1, :] = mean_in
        x_buf[layer, my_x, 2 * chunks + 1:2 * chunks + 2, :] = mean_out
        for d in x_devs:
            send(x_buf.at[layer, my_x], x_sem.at[layer], d, 1)

    def stage_x(layer):
        arrived(x_buf.at[layer, pl.ds(0, nx - 1)], x_sem.at[layer])
        y_buf[layer, my_y] = total(x_buf, layer, nx)
        for d in y_devs:
            send(y_buf.at[layer, my_y], y_sem.at[layer], d, 2)

    def stage_y(layer):
        arrived(y_buf.at[layer, pl.ds(0, ny - 1)], y_sem.at[layer])
        z_buf[layer, my_z] = total(y_buf, layer, ny)
        for d in z_devs:
            send(z_buf.at[layer, my_z], z_sem.at[layer], d, 3)

    def stage_z(layer):
        arrived(z_buf.at[layer, pl.ds(0, nz - 1)], z_sem.at[layer])
        tot = total(z_buf, layer, nz)
        low, high = tot[:half], tot[half:]
        new = beta * old_pack[layer] + low * (keep / n_side)
        new_pack[layer] = new
        mean = jnp.sqrt(jnp.sum(low[2 * chunks:2 * chunks + 2, :], axis=1, keepdims=True))
        u = lax.rsqrt(new) * jnp.where(first, mean[0:1], mean[1:2])
        u_v[layer] = u
        part = (high * u) * u
        fin_buf[layer, core, 0:1, :] = jnp.sum(jnp.where(first, part, 0.0), axis=0, keepdims=True)
        fin_buf[layer, core, 1:2, :] = jnp.sum(jnp.where(second, part, 0.0), axis=0, keepdims=True)
        fin_buf[layer, core, 2:4, :] = high[2 * chunks:2 * chunks + 2, :]
        fin_buf[layer, core, 4:, :] = jnp.zeros((4, LANES), jnp.float32)
        send(fin_buf.at[layer, core], fin_sem.at[layer], partner, 4)

    def stage_f(layer):
        arrived(fin_buf.at[layer, 0], fin_sem.at[layer])
        rms = jnp.sqrt(jnp.sum(total(fin_buf, layer, 2), axis=1, keepdims=True) / n_total)
        amount = hyper_s[1] * jnp.maximum(EPS_TWO, rms[2:4]) / jnp.maximum(1.0, rms[0:2] / hyper_s[2])
        fac_v[...] = u_v[layer] * jnp.where(first, amount[0:1], amount[1:2])
        for j in range(2):
            for k in range(chunks):
                cols = slice(k * LANES, (k + 1) * LANES)
                w_v[j, layer, :, cols] = w_v[j, layer, :, cols] - g_v[j, layer, :, cols] * fac_v[j * chunks + k:j * chunks + k + 1, :]

    def at(i, lag, stage, count):
        pl.when((i >= lag) & (i < count + lag))(lambda: stage(i - lag))

    def step(i, carry):
        at(i, 0, stage_a, layers)

        @pl.when(i == 1)
        def _():
            for c in big:
                c.wait()

        at(i, 1, stage_d, layers)
        at(i, 1 + LAG, stage_x, layers)
        at(i, 1 + 2 * LAG, stage_y, layers)
        at(i, 1 + 3 * LAG, stage_z, layers)
        at(i, 2 + 3 * LAG, stage_f, layers - 1)
        return carry

    lax.fori_loop(0, layers + 1 + 3 * LAG, step, 0)

    for layer in range(layers):
        for j in range(2):
            for k in range(chunks):
                lane_res[j, layer:layer + 1, k * LANES:(k + 1) * LANES] = new_pack[layer, j * chunks + k:j * chunks + k + 1, :]
            line = side_new[layer, j * depth:(j + 1) * depth, :depth]
            side_res[j, layer:layer + 1, :] = jnp.sum(jnp.where(eye, line, 0.0), axis=0, keepdims=True)
    stage_f(layers - 1)

    def sent(ref, k):
        pltpu.make_async_copy(ref, ref, send_sem.at[k]).wait()

    sent(pair_buf.at[:, 0], 0)
    sent(x_buf.at[:, pl.ds(0, nx - 1)], 1)
    sent(y_buf.at[:, pl.ds(0, ny - 1)], 2)
    sent(z_buf.at[:, pl.ds(0, nz - 1)], 3)
    sent(fin_buf.at[:, 0], 4)


def write_kernel(w_v, side_v, lane_v, o_w_in, o_side_in, o_lane_in, o_w_out, o_lane_out, o_side_out, sem):
    pairs = [(w_v.at[0], o_w_in), (w_v.at[1], o_w_out), (lane_v.at[0], o_lane_in), (lane_v.at[1], o_lane_out), (side_v.at[0], o_side_in), (side_v.at[1], o_side_out)]
    copies = [pltpu.make_async_copy(s, d, sem.at[i]) for i, (s, d) in enumerate(pairs)]
    for c in copies:
        c.start()
    for c in copies:
        c.wait()


def solution(mesh):
    dims = torus_dims(mesh.shape['row'])
    nz, ny, nx = dims
    tile_in = P(None, 'row', 'col')
    tile_out = P(None, 'col', 'row')
    lane_row = P(None, None, 'row')
    lane_col = P(None, None, 'col')
    vec_row = P(None, 'row')
    vec_col = P(None, 'col')

    def local_step(hyper_params, w_in, x_in, dy_in, row_in, col_in, w_out, x_out, dy_out, row_out, col_out):
        layers, depth, width = w_in.shape
        tokens = x_in.shape[1]
        chunks = width // LANES
        half = -(-(2 * chunks + 2) // 8) * 8
        f32 = jnp.float32
        turn = lambda v: jnp.swapaxes(v, 1, 2)
        vm = pltpu.VMEM
        dma = pltpu.SemaphoreType.DMA
        scratch = [
            pltpu.SMEM((3,), f32), vm((2, layers, depth, tokens), jnp.bfloat16), vm((SLOTS, tokens, width), jnp.bfloat16),
            vm((2, layers, depth, width), f32), vm((2, layers, depth), f32), vm((2, layers, width), f32),
            vm((layers, half, LANES), f32), vm((layers, 2 * depth, LANES), f32), vm((half, LANES), f32), vm((layers, half, LANES), f32), vm((layers, half, LANES), f32),
            vm((layers, 2, 2 * depth + 8, LANES), f32),
            vm((layers, nx, 2 * half, LANES), f32), vm((layers, ny, 2 * half, LANES), f32), vm((layers, nz, 2 * half, LANES), f32), vm((layers, 2, 8, LANES), f32),
            dma((9,)), dma((SLOTS,)), dma((5,)), dma((layers,)), dma((layers,)), dma((layers,)), dma((layers,)), dma((layers,)),
        ]
        in_vmem = pl.BlockSpec(memory_space=vm)
        anywhere = pl.BlockSpec(memory_space=pl.ANY)
        held = pl.pallas_call(
            functools.partial(kernel, dims),
            out_shape=(vm((2, layers, depth, width), f32), vm((2, layers, depth), f32), vm((2, layers, width), f32)),
            in_specs=[pl.BlockSpec(memory_space=pltpu.HBM)] * 11,
            out_specs=[in_vmem] * 3,
            scratch_shapes=scratch,
            name="adafactor_step",
            compiler_params=pltpu.CompilerParams(collective_id=0, has_side_effects=True, vmem_limit_bytes=VMEM_LIMIT),
        )(*[pltpu.with_memory_space_constraint(v, pltpu.HBM) for v in (hyper_params, turn(x_in), dy_in, w_in, row_in, col_in, turn(dy_out), x_out, turn(w_out), row_out, col_out)])
        shape = lambda *s: jax.ShapeDtypeStruct(s, f32)
        res = pl.pallas_call(
            write_kernel,
            out_shape=(shape(layers, depth, width), shape(layers, depth), shape(layers, width), shape(layers, depth, width), shape(layers, width), shape(layers, depth)),
            in_specs=[anywhere] * 3,
            out_specs=[anywhere] * 6,
            scratch_shapes=[dma((6,))],
            name="write_back",
            compiler_params=pltpu.CompilerParams(vmem_limit_bytes=4 * 1024 * 1024),
        )(*held)
        return res[0], res[1], res[2], turn(res[3]), res[4], res[5]

    return jax.shard_map(local_step, mesh=mesh, in_specs=(P(), tile_in, lane_row, lane_col, vec_row, vec_col, tile_out, lane_col, lane_row, vec_col, vec_row), out_specs=(tile_in, vec_row, vec_col, tile_out, vec_col, vec_row), check_vma=False)
```

```python
import functools

import jax
import jax.numpy as jnp
from jax import lax
from jax.experimental import pallas as pl
from jax.experimental.pallas import tpu as pltpu
from jax.sharding import PartitionSpec as P

EPS_ONE = 1e-30
EPS_TWO = 1e-3
MESH = pl.DeviceIdType.MESH
LANES = 128
SLOTS = 8
LAG = 5
LAG_D = 3
VMEM_LIMIT = 48 * 1024 * 1024


def torus_side(n_row):
    return round(n_row ** (1.0 / 3.0))


def kernel(side, hyper, a_in, b_in, w_in, side_in, lane_in, a_out, b_out, w_out, lane_out, side_out,
           w_v, side_res, lane_res,
           hyper_s, a_v, b_v, g_v, r_v, side_old, lane_old, old_pack, side_buf, side_out_buf, side_back,
           fac_v, new_pack, u_v, pair_buf, p_buf, fin_buf,
           load_sem, a_sem, ar_sem, b_sem, send_sem, so_sem, sb_sem, pair_sem, p_sem, g_sem, fin_sem):
    layers, depth, width = w_in.shape
    chunks = width // LANES
    half = chunks + 1
    n_row = side ** 3
    n_side = float(depth * n_row)
    n_lane = float(width * 2)
    n_total = n_side * n_lane

    row = lax.axis_index("row")
    core = lax.axis_index("col")

    def stride_of(d):
        return 1 + (side - 1) * d + ((side - 1) * (side - 1) * d * (d - 1)) // 2

    def pos_of(d):
        return lax.rem(row // stride_of(d), side)

    def moved(d, pos):
        return row + (pos - pos_of(d)) * stride_of(d)

    def pair(layer):
        kind = lax.rem(layer, 6)
        d = kind // 2
        flavour = lax.rem(kind, 2)
        pos = pos_of(d)
        role = lax.rem(pos, 2)
        mate = lax.rem(pos + (1 - 2 * role) * (1 - 2 * flavour) + side, side)
        return d, role, moved(d, mate)

    def dev(r, c):
        return {"row": r, "col": c}

    b_refs = (b_in, b_out)
    a_refs = (a_in, a_out)

    def b_start(layer):
        slot = lax.rem(layer, SLOTS)
        role = pair(layer)[1]
        for j in range(2):
            @pl.when(role == j)
            def _():
                pltpu.make_async_copy(b_refs[j].at[layer], b_v.at[slot], b_sem.at[slot]).start()

    small = [(hyper, hyper_s), (side_in, side_old.at[0]), (side_out, side_old.at[1]), (lane_in, lane_old.at[0]), (lane_out, lane_old.at[1])]
    small = [pltpu.make_async_copy(s, d, load_sem.at[i]) for i, (s, d) in enumerate(small)]
    big = [pltpu.make_async_copy(s, w_v.at[j], load_sem.at[len(small) + j]) for j, s in enumerate((w_in, w_out))]
    barrier = pltpu.get_barrier_semaphore()
    peers = [dev(moved(d, lax.rem(pos_of(d) + t, side)), core) for d in range(3) for t in range(1, side)] + [dev(row, 1 - core)]
    for d in peers:
        pl.semaphore_signal(barrier, inc=1, device_id=d, device_id_type=MESH)
    for c in small:
        c.start()

    def load_a(layer, carry):
        role = pair(layer)[1]
        for j in range(2):
            @pl.when(role == j)
            def _():
                pltpu.make_async_copy(a_refs[j].at[layer], a_v.at[layer, pl.ds(0, depth)], a_sem.at[layer]).start()
        return carry

    lax.fori_loop(0, layers, load_a, 0)
    for s in range(SLOTS):
        b_start(s)
        if s == 3:
            for c in big:
                c.start()
    for c in small:
        c.wait()

    beta = hyper_s[0]
    keep = 1.0 - beta
    eye = lax.broadcasted_iota(jnp.int32, (depth, depth), 0) == lax.broadcasted_iota(jnp.int32, (depth, depth), 1)
    half_id = lax.broadcasted_iota(jnp.int32, (half, LANES), 0)
    real = half_id < chunks
    left = lax.broadcasted_iota(jnp.int32, (1, LANES), 1) < LANES // 2

    def send(src, dst, recv, d, k):
        pltpu.make_async_remote_copy(src_ref=src, dst_ref=dst, send_sem=send_sem.at[k], recv_sem=recv, device_id=d, device_id_type=MESH).start()

    def arrived(ref, sem):
        pltpu.make_async_copy(ref, ref, sem).wait()

    pl.semaphore_wait(barrier, len(peers))

    def send_a(layer, carry):
        _, role, mate = pair(layer)
        for j in range(2):
            @pl.when(role == 1 - j)
            def _():
                send(a_refs[j].at[layer], a_v.at[layer, pl.ds(depth, depth)], ar_sem.at[layer], dev(mate, core), 0)
        return carry

    lax.fori_loop(0, layers, send_a, 0)

    for layer in range(layers):
        _, role, mate = pair(layer)
        column = []
        for j in range(2):
            for k in range(chunks):
                old_pack[layer, j, k:k + 1, :] = lane_old[j, layer:layer + 1, k * LANES:(k + 1) * LANES]
            old_pack[layer, j, chunks:, :] = jnp.ones((half - chunks, LANES), jnp.float32)
            line = jnp.broadcast_to(side_old[j, layer:layer + 1, :], (depth, depth))
            line = jnp.sum(jnp.where(eye, line, 0.0), axis=1, keepdims=True)
            column.append(jnp.broadcast_to(line, (depth, LANES)))
        side_buf[layer, :depth, :] = jnp.where(role == 0, column[0], column[1])
        side_out_buf[layer] = jnp.where(role == 0, column[1], column[0])
        send(side_out_buf.at[layer], side_buf.at[layer, pl.ds(depth, depth)], so_sem.at[layer], dev(mate, core), 1)
        line = jnp.sum(jnp.where(real, old_pack[layer, 1], 0.0), axis=0, keepdims=True)
        pair_buf[layer, core, 2 * depth:, :] = jnp.broadcast_to(line, (8, LANES))

    def stage_a(layer):
        d, role, mate = pair(layer)
        mine = p_buf.at[0, layer, pos_of(lax.rem(d + 1, 3))]
        slot = lax.rem(layer, SLOTS)
        arrived(a_v.at[layer, pl.ds(0, depth)], a_sem.at[layer])
        arrived(a_v.at[layer, pl.ds(0, depth)], ar_sem.at[layer])
        arrived(b_v.at[slot], b_sem.at[slot])
        grad = jnp.dot(a_v[layer], b_v[slot], preferred_element_type=jnp.float32)
        g_v[layer] = grad
        sq = grad * grad + EPS_ONE
        lane_part = jnp.sum(sq, axis=0, keepdims=True)
        part = sq[:, :LANES]
        for k in range(chunks):
            cols = slice(k * LANES, (k + 1) * LANES)
            if k:
                part = part + sq[:, cols]
            mine[k:k + 1, :] = lane_part[:, cols]
        pair_buf[layer, core, :2 * depth, :] = part
        send(pair_buf.at[layer, core], pair_buf.at[layer, core], pair_sem.at[layer], dev(row, 1 - core), 2)
        pl.when(layer + SLOTS < layers)(lambda: b_start(layer + SLOTS))

    def total(buf, count):
        out = buf[0]
        for s in range(1, count):
            out = out + buf[s]
        return out

    def stage_d(layer):
        d, role, mate = pair(layer)
        arrived(side_buf.at[layer, pl.ds(0, depth)], so_sem.at[layer])
        arrived(pair_buf.at[layer, 0], pair_sem.at[layer])
        both = total(pair_buf.at[layer], 2)
        side_sum = jnp.sum(both[:2 * depth], axis=1, keepdims=True)
        new = beta * side_buf[layer] + side_sum * (keep / n_lane)
        side_buf[layer] = new
        inv = lax.rsqrt(new)
        axis = lax.rem(d + 1, 3)
        me = pos_of(axis)
        mine = p_buf.at[0, layer, me]
        for k in range(chunks):
            cols = slice(k * LANES, (k + 1) * LANES)
            upd = g_v[layer, :, cols] * inv
            g_v[layer, :, cols] = upd
            mine[half + k:half + k + 1, :] = jnp.sum(upd * upd, axis=0, keepdims=True)
        w_sum = []
        for j in range(2):
            w_sq = None
            for k in range(chunks):
                wgt = w_v[j, layer, :, k * LANES:(k + 1) * LANES]
                w_sq = wgt * wgt if k == 0 else w_sq + wgt * wgt
            w_sum.append(jnp.sum(jnp.sum(w_sq, axis=0, keepdims=True), axis=1, keepdims=True) * (2.0 / LANES))
        mine[2 * half - 1:2 * half, :] = jnp.where(left, w_sum[0], w_sum[1])
        mean_in = jnp.sum(new, axis=0, keepdims=True) * (1.0 / (n_side * LANES))
        mean_out = jnp.broadcast_to(jnp.sum(side_sum, axis=0, keepdims=True), (1, LANES)) * (keep / (n_total * LANES))
        mean_out = mean_out + both[2 * depth:2 * depth + 1] * (beta / (n_lane * (n_row // 2)))
        mine[chunks:half, :] = jnp.where(role == 0, mean_in, mean_out)
        for t in range(1, side):
            send(mine, mine, p_sem.at[0, layer], dev(moved(axis, lax.rem(me + t, side)), core), 3)
        send(g_v.at[layer, pl.ds(depth, depth)], r_v.at[layer], g_sem.at[layer], dev(mate, core), 4)
        send(side_buf.at[layer, pl.ds(depth, depth)], side_back.at[layer], sb_sem.at[layer], dev(mate, core), 5)

    def stage_p(step, layer):
        arrived(p_buf.at[step, layer, pl.ds(0, side - 1)], p_sem.at[step, layer])
        axis = lax.rem(pair(layer)[0] + step + 2, 3)
        me = pos_of(axis)
        mine = p_buf.at[step + 1, layer, me]
        mine[...] = total(p_buf.at[step, layer], side)
        for t in range(1, side):
            send(mine, mine, p_sem.at[step + 1, layer], dev(moved(axis, lax.rem(me + t, side)), core), 6 + step)

    def stage_z(layer):
        arrived(p_buf.at[2, layer, pl.ds(0, side - 1)], p_sem.at[2, layer])
        weights = None
        for j in range(2):
            low = p_buf[2, layer, j, :half]
            high = p_buf[2, layer, j, half:]
            for s in range(j + 2, side, 2):
                low = low + p_buf[2, layer, s, :half]
                high = high + p_buf[2, layer, s, half:]
            new = jnp.where(real, beta * old_pack[layer, j] + low * (keep / n_side), 1.0)
            new_pack[layer, j] = new
            mean = jnp.sum(low[chunks:half], axis=1, keepdims=True)
            u = lax.rsqrt(new) * jnp.sqrt(mean)
            u_v[layer, j] = u
            fin_buf[layer, core, j:j + 1, :] = jnp.sum(jnp.where(real, (high * u) * u, 0.0), axis=0, keepdims=True)
            weights = high[half - 1:half] if j == 0 else weights + high[half - 1:half]
        fin_buf[layer, core, 2:3, :] = jnp.where(left, weights, 0.0)
        fin_buf[layer, core, 3:4, :] = jnp.where(left, 0.0, weights)
        fin_buf[layer, core, 4:, :] = jnp.zeros((4, LANES), jnp.float32)
        send(fin_buf.at[layer, core], fin_buf.at[layer, core], fin_sem.at[layer], dev(row, 1 - core), 8)

    def stage_f(layer):
        role = pair(layer)[1]
        arrived(r_v.at[layer], g_sem.at[layer])
        arrived(fin_buf.at[layer, 0], fin_sem.at[layer])
        rms = jnp.sqrt(jnp.sum(total(fin_buf.at[layer], 2), axis=1, keepdims=True) / n_total)
        amount = hyper_s[1] * jnp.maximum(EPS_TWO, rms[2:4]) / jnp.maximum(1.0, rms[0:2] / hyper_s[2])
        for j in range(2):
            fac_v[j] = u_v[layer, j] * amount[j:j + 1]
        for k in range(chunks):
            cols = slice(k * LANES, (k + 1) * LANES)
            w_v[role, layer, :, cols] = w_v[role, layer, :, cols] - g_v[layer, :depth, cols] * fac_v[role, k:k + 1, :]
            w_v[1 - role, layer, :, cols] = w_v[1 - role, layer, :, cols] - r_v[layer, :, cols] * fac_v[1 - role, k:k + 1, :]

    def at(i, lag, stage, count):
        pl.when((i >= lag) & (i < count + lag))(lambda: stage(i - lag))

    lag_z = LAG_D + 3 * LAG

    def step(i, carry):
        at(i, 0, stage_a, layers)

        @pl.when(i == LAG_D)
        def _():
            for c in big:
                c.wait()

        at(i, LAG_D, stage_d, layers)
        at(i, LAG_D + LAG, functools.partial(stage_p, 0), layers)
        at(i, LAG_D + 2 * LAG, functools.partial(stage_p, 1), layers)
        at(i, lag_z, stage_z, layers)
        at(i, lag_z + 1, stage_f, layers - 1)
        return carry

    lax.fori_loop(0, layers + lag_z, step, 0)

    for layer in range(layers):
        role = pair(layer)[1]
        arrived(side_back.at[layer], sb_sem.at[layer])
        for j in range(2):
            for k in range(chunks):
                lane_res[j, layer:layer + 1, k * LANES:(k + 1) * LANES] = new_pack[layer, j, k:k + 1, :]
        side_res[role, layer:layer + 1, :] = jnp.sum(jnp.where(eye, side_buf[layer, :depth, :depth], 0.0), axis=0, keepdims=True)
        side_res[1 - role, layer:layer + 1, :] = jnp.sum(jnp.where(eye, side_back[layer, :, :depth], 0.0), axis=0, keepdims=True)
    stage_f(layers - 1)

    def sent(ref, k):
        pltpu.make_async_copy(ref, ref, send_sem.at[k]).wait()

    sent(a_v.at[:, pl.ds(0, depth)], 0)
    sent(side_out_buf, 1)
    sent(pair_buf.at[:, 0], 2)
    sent(p_buf.at[0, :, pl.ds(0, side - 1)], 3)
    sent(r_v, 4)
    sent(side_back, 5)
    sent(p_buf.at[1, :, pl.ds(0, side - 1)], 6)
    sent(p_buf.at[2, :, pl.ds(0, side - 1)], 7)
    sent(fin_buf.at[:, 0], 8)


def write_kernel(w_v, side_v, lane_v, o_w_in, o_side_in, o_lane_in, o_w_out, o_lane_out, o_side_out, sem):
    pairs = [(w_v.at[0], o_w_in), (w_v.at[1], o_w_out), (lane_v.at[0], o_lane_in), (lane_v.at[1], o_lane_out), (side_v.at[0], o_side_in), (side_v.at[1], o_side_out)]
    copies = [pltpu.make_async_copy(s, d, sem.at[i]) for i, (s, d) in enumerate(pairs)]
    for c in copies:
        c.start()
    for c in copies:
        c.wait()


def solution(mesh):
    side = torus_side(mesh.shape['row'])
    tile_in = P(None, 'row', 'col')
    tile_out = P(None, 'col', 'row')
    lane_row = P(None, None, 'row')
    lane_col = P(None, None, 'col')
    vec_row = P(None, 'row')
    vec_col = P(None, 'col')

    def local_step(hyper_params, w_in, x_in, dy_in, row_in, col_in, w_out, x_out, dy_out, row_out, col_out):
        layers, depth, width = w_in.shape
        tokens = x_in.shape[1]
        chunks = width // LANES
        half = chunks + 1
        f32 = jnp.float32
        turn = lambda v: jnp.swapaxes(v, 1, 2)
        vm = pltpu.VMEM
        dma = pltpu.SemaphoreType.DMA
        scratch = [
            pltpu.SMEM((3,), f32), vm((layers, 2 * depth, tokens), jnp.bfloat16), vm((SLOTS, tokens, width), jnp.bfloat16),
            vm((layers, 2 * depth, width), f32), vm((layers, depth, width), f32),
            vm((2, layers, depth), f32), vm((2, layers, width), f32), vm((layers, 2, half, LANES), f32),
            vm((layers, 2 * depth, LANES), f32), vm((layers, depth, LANES), f32), vm((layers, depth, LANES), f32),
            vm((2, half, LANES), f32), vm((layers, 2, half, LANES), f32), vm((layers, 2, half, LANES), f32),
            vm((layers, 2, 2 * depth + 8, LANES), f32), vm((3, layers, side, 2 * half, LANES), f32), vm((layers, 2, 8, LANES), f32),
            dma((7,)), dma((layers,)), dma((layers,)), dma((SLOTS,)), dma((9,)), dma((layers,)), dma((layers,)), dma((layers,)), dma((3, layers)), dma((layers,)), dma((layers,)),
        ]
        in_vmem = pl.BlockSpec(memory_space=vm)
        anywhere = pl.BlockSpec(memory_space=pl.ANY)
        held = pl.pallas_call(
            functools.partial(kernel, side),
            out_shape=(vm((2, layers, depth, width), f32), vm((2, layers, depth), f32), vm((2, layers, width), f32)),
            in_specs=[pl.BlockSpec(memory_space=pltpu.HBM)] * 11,
            out_specs=[in_vmem] * 3,
            scratch_shapes=scratch,
            name="adafactor_step",
            compiler_params=pltpu.CompilerParams(collective_id=0, has_side_effects=True, vmem_limit_bytes=VMEM_LIMIT),
        )(*[pltpu.with_memory_space_constraint(v, pltpu.HBM) for v in (hyper_params, turn(x_in), dy_in, w_in, row_in, col_in, turn(dy_out), x_out, turn(w_out), row_out, col_out)])
        shape = lambda *s: jax.ShapeDtypeStruct(s, f32)
        res = pl.pallas_call(
            write_kernel,
            out_shape=(shape(layers, depth, width), shape(layers, depth), shape(layers, width), shape(layers, depth, width), shape(layers, width), shape(layers, depth)),
            in_specs=[anywhere] * 3,
            out_specs=[anywhere] * 6,
            scratch_shapes=[dma((6,))],
            name="write_back",
            compiler_params=pltpu.CompilerParams(vmem_limit_bytes=4 * 1024 * 1024),
        )(*held)
        return res[0], res[1], res[2], turn(res[3]), res[4], res[5]

    return jax.shard_map(local_step, mesh=mesh, in_specs=(P(), tile_in, lane_row, lane_col, vec_row, vec_col, tile_out, lane_col, lane_row, vec_col, vec_row), out_specs=(tile_in, vec_row, vec_col, tile_out, vec_col, vec_row), check_vma=False)
```

```python
import functools

import jax
import jax.numpy as jnp
from jax import lax
from jax.experimental import pallas as pl
from jax.experimental.pallas import tpu as pltpu
from jax.sharding import PartitionSpec as P

EPS_ONE = 1e-30
EPS_TWO = 1e-3
MESH = pl.DeviceIdType.MESH
LANES = 128
SLOTS = 6
LAG = 7
LAG_D = 2
VMEM_LIMIT = 48 * 1024 * 1024


def torus_side(n_row):
    return round(n_row ** (1.0 / 3.0))


def kernel(side, hyper, a_in, b_in, w_in, side_in, lane_in, a_out, b_out, w_out, lane_out, side_out,
           w_v, side_res, lane_res,
           hyper_s, a_v, ax_v, b_v, g_v, r_v, side_old, lane_old, old_pack, side_buf, side_out_buf, side_back,
           fac_v, new_pack, u_v, pair_buf, p_buf, fin_buf,
           load_sem, a_sem, ar_sem, ax_sem, w_sem, b_sem, send_sem, so_sem, sb_sem, pair_sem, p_sem, g_sem, fin_sem):
    layers, depth, width = w_in.shape
    chunks = width // LANES
    half = chunks + 1
    n_row = side ** 3
    n_side = float(depth * n_row)
    n_lane = float(width * 2)
    n_total = n_side * n_lane

    row = lax.axis_index("row")
    core = lax.axis_index("col")

    def stride_of(d):
        return 1 + (side - 1) * d + ((side - 1) * (side - 1) * d * (d - 1)) // 2

    def pos_of(d):
        return lax.rem(row // stride_of(d), side)

    def moved(d, pos):
        return row + (pos - pos_of(d)) * stride_of(d)

    def pair(layer):
        kind = lax.rem(layer, 6)
        d = kind // 2
        flavour = lax.rem(kind, 2)
        pos = pos_of(d)
        role = lax.rem(pos, 2)
        mate = lax.rem(pos + (1 - 2 * role) * (1 - 2 * flavour) + side, side)
        return d, role, moved(d, mate)

    def dev(r, c):
        return {"row": r, "col": c}

    b_refs = (b_in, b_out)
    a_refs = (a_in, a_out)
    w_refs = (w_in, w_out)

    def b_start(layer):
        slot = lax.rem(layer, SLOTS)
        role = pair(layer)[1]
        for j in range(2):
            @pl.when(role == j)
            def _():
                pltpu.make_async_copy(b_refs[j].at[layer], b_v.at[slot], b_sem.at[slot]).start()
            pltpu.make_async_copy(w_refs[j].at[layer], w_v.at[j, layer], w_sem.at[layer]).start()

    small = [(hyper, hyper_s), (side_in, side_old.at[0]), (side_out, side_old.at[1]), (lane_in, lane_old.at[0]), (lane_out, lane_old.at[1])]
    small = [pltpu.make_async_copy(s, d, load_sem.at[i]) for i, (s, d) in enumerate(small)]
    barrier = pltpu.get_barrier_semaphore()
    peers = [dev(moved(d, lax.rem(pos_of(d) + t, side)), core) for d in range(3) for t in range(1, side)] + [dev(row, 1 - core)]
    for d in peers:
        pl.semaphore_signal(barrier, inc=1, device_id=d, device_id_type=MESH)
    for c in small:
        c.start()

    def load_a(layer, carry):
        role = pair(layer)[1]
        for j in range(2):
            @pl.when(role == j)
            def _():
                pltpu.make_async_copy(a_refs[1 - j].at[layer], ax_v.at[layer], ax_sem.at[layer]).start()
                pltpu.make_async_copy(a_refs[j].at[layer], a_v.at[layer, pl.ds(0, depth)], a_sem.at[layer]).start()
        return carry

    lax.fori_loop(0, layers, load_a, 0)
    for s in range(SLOTS):
        b_start(s)
    for c in small:
        c.wait()

    beta = hyper_s[0]
    keep = 1.0 - beta
    eye = lax.broadcasted_iota(jnp.int32, (depth, depth), 0) == lax.broadcasted_iota(jnp.int32, (depth, depth), 1)
    half_id = lax.broadcasted_iota(jnp.int32, (half, LANES), 0)
    real = half_id < chunks
    left = lax.broadcasted_iota(jnp.int32, (1, LANES), 1) < LANES // 2

    def send(src, dst, recv, d, k):
        pltpu.make_async_remote_copy(src_ref=src, dst_ref=dst, send_sem=send_sem.at[k], recv_sem=recv, device_id=d, device_id_type=MESH).start()

    def arrived(ref, sem):
        pltpu.make_async_copy(ref, ref, sem).wait()

    old_sum = lane_old[1, :, :LANES]
    for k in range(1, chunks):
        old_sum = old_sum + lane_old[1, :, k * LANES:(k + 1) * LANES]
    for layer in range(layers):
        role = pair(layer)[1]
        column = []
        for j in range(2):
            line = jnp.broadcast_to(side_old[j, layer:layer + 1, :], (depth, depth))
            line = jnp.sum(jnp.where(eye, line, 0.0), axis=1, keepdims=True)
            column.append(jnp.broadcast_to(line, (depth, LANES)))
        side_buf[layer, :depth, :] = jnp.where(role == 0, column[0], column[1])
        side_out_buf[layer] = jnp.where(role == 0, column[1], column[0])
        pair_buf[layer, core, 2 * depth:, :] = jnp.broadcast_to(old_sum[layer:layer + 1], (8, LANES))
    pl.semaphore_wait(barrier, len(peers))

    def send_a(layer, carry):
        _, role, mate = pair(layer)
        arrived(ax_v.at[layer], ax_sem.at[layer])
        send(ax_v.at[layer], a_v.at[layer, pl.ds(depth, depth)], ar_sem.at[layer], dev(mate, core), 0)
        send(side_out_buf.at[layer], side_buf.at[layer, pl.ds(depth, depth)], so_sem.at[layer], dev(mate, core), 1)
        return carry

    lax.fori_loop(0, layers, send_a, 0)

    def wait_a(layer):
        slot = lax.rem(layer, SLOTS)
        arrived(a_v.at[layer, pl.ds(0, depth)], a_sem.at[layer])
        arrived(a_v.at[layer, pl.ds(0, depth)], ar_sem.at[layer])
        arrived(b_v.at[slot], b_sem.at[slot])

    def work_a(layer):
        d, role, mate = pair(layer)
        mine = p_buf.at[0, layer, pos_of(lax.rem(d + 1, 3))]
        slot = lax.rem(layer, SLOTS)
        grad = jnp.dot(a_v[layer], b_v[slot], preferred_element_type=jnp.float32)
        g_v[layer] = grad
        sq = grad * grad + EPS_ONE
        lane_part = jnp.sum(sq, axis=0, keepdims=True)
        part = sq[:, :LANES]
        for k in range(chunks):
            cols = slice(k * LANES, (k + 1) * LANES)
            if k:
                part = part + sq[:, cols]
            mine[k:k + 1, :] = lane_part[:, cols]
        pair_buf[layer, core, :2 * depth, :] = part

    def send_pair(layer):
        send(pair_buf.at[layer, core], pair_buf.at[layer, core], pair_sem.at[layer], dev(row, 1 - core), 2)

    def total(buf, count):
        out = buf[0]
        for s in range(1, count):
            out = out + buf[s]
        return out

    def wait_d(layer):
        arrived(w_v.at[:, layer], w_sem.at[layer])
        arrived(side_buf.at[layer, pl.ds(0, depth)], so_sem.at[layer])
        arrived(pair_buf.at[layer, 0], pair_sem.at[layer])

    def work_d(layer):
        d, role, mate = pair(layer)
        both = total(pair_buf.at[layer], 2)
        side_sum = jnp.sum(both[:2 * depth], axis=1, keepdims=True)
        new = beta * side_buf[layer] + side_sum * (keep / n_lane)
        side_buf[layer] = new
        inv = lax.rsqrt(new)
        axis = lax.rem(d + 1, 3)
        me = pos_of(axis)
        mine = p_buf.at[0, layer, me]
        for k in range(chunks):
            cols = slice(k * LANES, (k + 1) * LANES)
            upd = g_v[layer, :, cols] * inv
            g_v[layer, :, cols] = upd
            mine[half + k:half + k + 1, :] = jnp.sum(upd * upd, axis=0, keepdims=True)
        w_sum = []
        for j in range(2):
            w_sq = None
            for k in range(chunks):
                wgt = w_v[j, layer, :, k * LANES:(k + 1) * LANES]
                w_sq = wgt * wgt if k == 0 else w_sq + wgt * wgt
            w_sum.append(jnp.sum(jnp.sum(w_sq, axis=0, keepdims=True), axis=1, keepdims=True) * (2.0 / LANES))
        mine[2 * half - 1:2 * half, :] = jnp.where(left, w_sum[0], w_sum[1])
        mean_in = jnp.sum(new, axis=0, keepdims=True) * (1.0 / (n_side * LANES))
        mean_out = jnp.broadcast_to(jnp.sum(side_sum, axis=0, keepdims=True), (1, LANES)) * (keep / (n_total * LANES))
        mean_out = mean_out + both[2 * depth:2 * depth + 1] * (beta / (n_lane * (n_row // 2)))
        mine[chunks:half, :] = jnp.where(role == 0, mean_in, mean_out)

    def send_d(layer):
        d, role, mate = pair(layer)
        axis = lax.rem(d + 1, 3)
        me = pos_of(axis)
        mine = p_buf.at[0, layer, me]
        for t in range(1, side):
            send(mine, mine, p_sem.at[0, layer], dev(moved(axis, lax.rem(me + t, side)), core), 3)
        send(g_v.at[layer, pl.ds(depth, depth)], r_v.at[layer], g_sem.at[layer], dev(mate, core), 4)
        send(side_buf.at[layer, pl.ds(depth, depth)], side_back.at[layer], sb_sem.at[layer], dev(mate, core), 5)

    def stage_p(step, layer):
        arrived(p_buf.at[step, layer, pl.ds(0, side - 1)], p_sem.at[step, layer])
        axis = lax.rem(pair(layer)[0] + step + 2, 3)
        me = pos_of(axis)
        mine = p_buf.at[step + 1, layer, me]
        mine[...] = total(p_buf.at[step, layer], side)
        for t in range(1, side):
            send(mine, mine, p_sem.at[step + 1, layer], dev(moved(axis, lax.rem(me + t, side)), core), 6 + step)

    def stage_z(layer):
        arrived(p_buf.at[2, layer, pl.ds(0, side - 1)], p_sem.at[2, layer])
        weights = None
        for j in range(2):
            low = p_buf[2, layer, j, :half]
            high = p_buf[2, layer, j, half:]
            for s in range(j + 2, side, 2):
                low = low + p_buf[2, layer, s, :half]
                high = high + p_buf[2, layer, s, half:]
            new = jnp.where(real, beta * old_pack[layer, j] + low * (keep / n_side), 1.0)
            new_pack[layer, j] = new
            mean = jnp.sum(low[chunks:half], axis=1, keepdims=True)
            u = lax.rsqrt(new) * jnp.sqrt(mean)
            u_v[layer, j] = u
            fin_buf[layer, core, j:j + 1, :] = jnp.sum(jnp.where(real, (high * u) * u, 0.0), axis=0, keepdims=True)
            weights = high[half - 1:half] if j == 0 else weights + high[half - 1:half]
        fin_buf[layer, core, 2:3, :] = jnp.where(left, weights, 0.0)
        fin_buf[layer, core, 3:4, :] = jnp.where(left, 0.0, weights)
        fin_buf[layer, core, 4:, :] = jnp.zeros((4, LANES), jnp.float32)
        send(fin_buf.at[layer, core], fin_buf.at[layer, core], fin_sem.at[layer], dev(row, 1 - core), 8)

    def stage_f(layer):
        role = pair(layer)[1]
        arrived(r_v.at[layer], g_sem.at[layer])
        arrived(fin_buf.at[layer, 0], fin_sem.at[layer])
        rms = jnp.sqrt(jnp.sum(total(fin_buf.at[layer], 2), axis=1, keepdims=True) / n_total)
        amount = hyper_s[1] * jnp.maximum(EPS_TWO, rms[2:4]) / jnp.maximum(1.0, rms[0:2] / hyper_s[2])
        for j in range(2):
            fac_v[j] = u_v[layer, j] * amount[j:j + 1]
        for k in range(chunks):
            cols = slice(k * LANES, (k + 1) * LANES)
            w_v[role, layer, :, cols] = w_v[role, layer, :, cols] - g_v[layer, :depth, cols] * fac_v[role, k:k + 1, :]
            w_v[1 - role, layer, :, cols] = w_v[1 - role, layer, :, cols] - r_v[layer, :, cols] * fac_v[1 - role, k:k + 1, :]

    def at(i, lag, stage, count):
        pl.when((i >= lag) & (i < count + lag))(lambda: stage(i - lag))

    lag_z = LAG_D + 3 * LAG

    def exchange(i):
        at(i, LAG_D + LAG, functools.partial(stage_p, 0), layers)
        at(i, LAG_D + 2 * LAG, functools.partial(stage_p, 1), layers)
        at(i, lag_z, stage_z, layers)
        at(i, lag_z + 1, stage_f, layers - 1)

    def fill(i, carry):
        wait_a(i)
        work_a(i)
        send_pair(i)
        pl.when(i + SLOTS < layers)(lambda: b_start(i + SLOTS))
        return carry

    def steady(i, carry):
        wait_d(i - LAG_D)
        wait_a(i)
        work_d(i - LAG_D)
        work_a(i)
        send_pair(i)
        send_d(i - LAG_D)
        pl.when(i + SLOTS < layers)(lambda: b_start(i + SLOTS))
        exchange(i)
        return carry

    def drain(i, carry):
        @pl.when(i < layers + LAG_D)
        def _():
            wait_d(i - LAG_D)
            work_d(i - LAG_D)
            send_d(i - LAG_D)

        exchange(i)
        return carry

    lax.fori_loop(0, LAG_D, fill, 0)
    for layer in range(layers):
        for j in range(2):
            for k in range(chunks):
                old_pack[layer, j, k:k + 1, :] = lane_old[j, layer:layer + 1, k * LANES:(k + 1) * LANES]
            old_pack[layer, j, chunks:, :] = jnp.ones((half - chunks, LANES), jnp.float32)
    lax.fori_loop(LAG_D, layers, steady, 0)
    lax.fori_loop(layers, layers + lag_z, drain, 0)

    for layer in range(layers):
        role = pair(layer)[1]
        arrived(side_back.at[layer], sb_sem.at[layer])
        for j in range(2):
            for k in range(chunks):
                lane_res[j, layer:layer + 1, k * LANES:(k + 1) * LANES] = new_pack[layer, j, k:k + 1, :]
        side_res[role, layer:layer + 1, :] = jnp.sum(jnp.where(eye, side_buf[layer, :depth, :depth], 0.0), axis=0, keepdims=True)
        side_res[1 - role, layer:layer + 1, :] = jnp.sum(jnp.where(eye, side_back[layer, :, :depth], 0.0), axis=0, keepdims=True)
    stage_f(layers - 1)

    def sent(ref, k):
        pltpu.make_async_copy(ref, ref, send_sem.at[k]).wait()

    sent(a_v.at[:, pl.ds(0, depth)], 0)
    sent(side_out_buf, 1)
    sent(pair_buf.at[:, 0], 2)
    sent(p_buf.at[0, :, pl.ds(0, side - 1)], 3)
    sent(r_v, 4)
    sent(side_back, 5)
    sent(p_buf.at[1, :, pl.ds(0, side - 1)], 6)
    sent(p_buf.at[2, :, pl.ds(0, side - 1)], 7)
    sent(fin_buf.at[:, 0], 8)


def write_kernel(w_v, side_v, lane_v, o_w_in, o_side_in, o_lane_in, o_w_out, o_lane_out, o_side_out, sem):
    pairs = [(w_v.at[0], o_w_in), (w_v.at[1], o_w_out), (lane_v.at[0], o_lane_in), (lane_v.at[1], o_lane_out), (side_v.at[0], o_side_in), (side_v.at[1], o_side_out)]
    copies = [pltpu.make_async_copy(s, d, sem.at[i]) for i, (s, d) in enumerate(pairs)]
    for c in copies:
        c.start()
    for c in copies:
        c.wait()


def solution(mesh):
    side = torus_side(mesh.shape['row'])
    tile_in = P(None, 'row', 'col')
    tile_out = P(None, 'col', 'row')
    lane_row = P(None, None, 'row')
    lane_col = P(None, None, 'col')
    vec_row = P(None, 'row')
    vec_col = P(None, 'col')

    def local_step(hyper_params, w_in, x_in, dy_in, row_in, col_in, w_out, x_out, dy_out, row_out, col_out):
        layers, depth, width = w_in.shape
        tokens = x_in.shape[1]
        chunks = width // LANES
        half = chunks + 1
        f32 = jnp.float32
        turn = lambda v: jnp.swapaxes(v, 1, 2)
        vm = pltpu.VMEM
        dma = pltpu.SemaphoreType.DMA
        scratch = [
            pltpu.SMEM((3,), f32), vm((layers, 2 * depth, tokens), jnp.bfloat16), vm((layers, depth, tokens), jnp.bfloat16), vm((SLOTS, tokens, width), jnp.bfloat16),
            vm((layers, 2 * depth, width), f32), vm((layers, depth, width), f32),
            vm((2, layers, depth), f32), vm((2, layers, width), f32), vm((layers, 2, half, LANES), f32),
            vm((layers, 2 * depth, LANES), f32), vm((layers, depth, LANES), f32), vm((layers, depth, LANES), f32),
            vm((2, half, LANES), f32), vm((layers, 2, half, LANES), f32), vm((layers, 2, half, LANES), f32),
            vm((layers, 2, 2 * depth + 8, LANES), f32), vm((3, layers, side, 2 * half, LANES), f32), vm((layers, 2, 8, LANES), f32),
            dma((5,)), dma((layers,)), dma((layers,)), dma((layers,)), dma((layers,)), dma((SLOTS,)), dma((9,)), dma((layers,)), dma((layers,)), dma((layers,)), dma((3, layers)), dma((layers,)), dma((layers,)),
        ]
        in_vmem = pl.BlockSpec(memory_space=vm)
        anywhere = pl.BlockSpec(memory_space=pl.ANY)
        held = pl.pallas_call(
            functools.partial(kernel, side),
            out_shape=(vm((2, layers, depth, width), f32), vm((2, layers, depth), f32), vm((2, layers, width), f32)),
            in_specs=[pl.BlockSpec(memory_space=pltpu.HBM)] * 11,
            out_specs=[in_vmem] * 3,
            scratch_shapes=scratch,
            name="adafactor_step",
            compiler_params=pltpu.CompilerParams(collective_id=0, has_side_effects=True, vmem_limit_bytes=VMEM_LIMIT),
        )(*[pltpu.with_memory_space_constraint(v, pltpu.HBM) for v in (hyper_params, turn(x_in), dy_in, w_in, row_in, col_in, turn(dy_out), x_out, turn(w_out), row_out, col_out)])
        shape = lambda *s: jax.ShapeDtypeStruct(s, f32)
        res = pl.pallas_call(
            write_kernel,
            out_shape=(shape(layers, depth, width), shape(layers, depth), shape(layers, width), shape(layers, depth, width), shape(layers, width), shape(layers, depth)),
            in_specs=[anywhere] * 3,
            out_specs=[anywhere] * 6,
            scratch_shapes=[dma((6,))],
            name="write_back",
            compiler_params=pltpu.CompilerParams(vmem_limit_bytes=4 * 1024 * 1024),
        )(*held)
        return res[0], res[1], res[2], turn(res[3]), res[4], res[5]

    return jax.shard_map(local_step, mesh=mesh, in_specs=(P(), tile_in, lane_row, lane_col, vec_row, vec_col, tile_out, lane_col, lane_row, vec_col, vec_row), out_specs=(tile_in, vec_row, vec_col, tile_out, vec_col, vec_row), check_vma=False)
```

```python
import functools

import jax
import jax.numpy as jnp
from jax import lax
from jax.experimental import pallas as pl
from jax.experimental.pallas import tpu as pltpu
from jax.sharding import PartitionSpec as P

EPS_ONE = 1e-30
EPS_TWO = 1e-3
MESH = pl.DeviceIdType.MESH
LANES = 128
SLOTS = 6
LAG = 7
LAG_D = 3
EARLY = 6
VMEM_LIMIT = 48 * 1024 * 1024


def torus_side(n_row):
    return round(n_row ** (1.0 / 3.0))


def kernel(side, hyper, a_in, b_in, w_in, side_in, lane_in, a_out, b_out, w_out, lane_out, side_out,
           w_v, side_res, lane_res,
           hyper_s, a_v, ax_v, b_v, g_v, r_v, side_old, lane_old, old_pack, side_buf, side_out_buf, side_back,
           fac_v, new_pack, u_v, pair_buf, p_buf, fin_buf,
           load_sem, a_sem, ar_sem, ax_sem, w_sem, b_sem, send_sem, so_sem, sb_sem, pair_sem, p_sem, g_sem, fin_sem):
    layers, depth, width = w_in.shape
    chunks = width // LANES
    half = chunks + 1
    n_row = side ** 3
    n_side = float(depth * n_row)
    n_lane = float(width * 2)
    n_total = n_side * n_lane

    row = lax.axis_index("row")
    core = lax.axis_index("col")

    def stride_of(d):
        return 1 + (side - 1) * d + ((side - 1) * (side - 1) * d * (d - 1)) // 2

    def pos_of(d):
        return lax.rem(row // stride_of(d), side)

    def moved(d, pos):
        return row + (pos - pos_of(d)) * stride_of(d)

    def pair(layer):
        kind = lax.rem(layer, 6)
        d = kind // 2
        flavour = lax.rem(kind, 2)
        pos = pos_of(d)
        role = lax.rem(pos, 2)
        mate = lax.rem(pos + (1 - 2 * role) * (1 - 2 * flavour) + side, side)
        return d, role, moved(d, mate)

    def dev(r, c):
        return {"row": r, "col": c}

    b_refs = (b_in, b_out)
    a_refs = (a_in, a_out)
    w_refs = (w_in, w_out)

    def b_start(layer):
        slot = lax.rem(layer, SLOTS)
        role = pair(layer)[1]
        for j in range(2):
            @pl.when(role == j)
            def _():
                pltpu.make_async_copy(b_refs[j].at[layer], b_v.at[slot], b_sem.at[slot]).start()
            pltpu.make_async_copy(w_refs[j].at[layer], w_v.at[j, layer], w_sem.at[layer]).start()

    small = [(hyper, hyper_s), (side_in, side_old.at[0]), (side_out, side_old.at[1]), (lane_in, lane_old.at[0]), (lane_out, lane_old.at[1])]
    small = [pltpu.make_async_copy(s, d, load_sem.at[i]) for i, (s, d) in enumerate(small)]
    barrier = pltpu.get_barrier_semaphore()
    peers = [dev(moved(d, lax.rem(pos_of(d) + t, side)), core) for d in range(3) for t in range(1, side)] + [dev(row, 1 - core)]
    for d in peers:
        pl.semaphore_signal(barrier, inc=1, device_id=d, device_id_type=MESH)
    for c in small:
        c.start()

    def load_a(layer, carry):
        role = pair(layer)[1]
        for j in range(2):
            @pl.when(role == j)
            def _():
                pltpu.make_async_copy(a_refs[1 - j].at[layer], ax_v.at[layer], ax_sem.at[layer]).start()
                pltpu.make_async_copy(a_refs[j].at[layer], a_v.at[layer, pl.ds(0, depth)], a_sem.at[layer]).start()
        return carry

    lax.fori_loop(0, layers, load_a, 0)
    for s in range(SLOTS):
        b_start(s)

    def send(src, dst, recv, d, k):
        pltpu.make_async_remote_copy(src_ref=src, dst_ref=dst, send_sem=send_sem.at[k], recv_sem=recv, device_id=d, device_id_type=MESH).start()

    def arrived(ref, sem):
        pltpu.make_async_copy(ref, ref, sem).wait()

    def send_a(layer):
        arrived(ax_v.at[layer], ax_sem.at[layer])
        send(ax_v.at[layer], a_v.at[layer, pl.ds(depth, depth)], ar_sem.at[layer], dev(pair(layer)[2], core), 0)

    pl.semaphore_wait(barrier, len(peers))
    for layer in range(EARLY):
        send_a(layer)
    for c in small:
        c.wait()

    beta = hyper_s[0]
    keep = 1.0 - beta
    eye = lax.broadcasted_iota(jnp.int32, (depth, depth), 0) == lax.broadcasted_iota(jnp.int32, (depth, depth), 1)
    half_id = lax.broadcasted_iota(jnp.int32, (half, LANES), 0)
    real = half_id < chunks
    left = lax.broadcasted_iota(jnp.int32, (1, LANES), 1) < LANES // 2

    old_sum = lane_old[1, :, :LANES]
    for k in range(1, chunks):
        old_sum = old_sum + lane_old[1, :, k * LANES:(k + 1) * LANES]
    for layer in range(layers):
        role = pair(layer)[1]
        column = []
        for j in range(2):
            line = jnp.broadcast_to(side_old[j, layer:layer + 1, :], (depth, depth))
            line = jnp.sum(jnp.where(eye, line, 0.0), axis=1, keepdims=True)
            column.append(jnp.broadcast_to(line, (depth, LANES)))
        side_buf[layer, :depth, :] = jnp.where(role == 0, column[0], column[1])
        side_out_buf[layer] = jnp.where(role == 0, column[1], column[0])
        pair_buf[layer, core, 2 * depth:, :] = jnp.broadcast_to(old_sum[layer:layer + 1], (8, LANES))

    def send_side(layer, carry):
        mate = pair(layer)[2]
        send(side_out_buf.at[layer], side_buf.at[layer, pl.ds(depth, depth)], so_sem.at[layer], dev(mate, core), 1)
        pl.when(layer >= EARLY)(lambda: send_a(layer))
        return carry

    lax.fori_loop(0, layers, send_side, 0)

    def wait_a(layer):
        slot = lax.rem(layer, SLOTS)
        arrived(a_v.at[layer, pl.ds(0, depth)], a_sem.at[layer])
        arrived(a_v.at[layer, pl.ds(0, depth)], ar_sem.at[layer])
        arrived(b_v.at[slot], b_sem.at[slot])

    def work_a(layer):
        d, role, mate = pair(layer)
        mine = p_buf.at[0, layer, pos_of(lax.rem(d + 1, 3))]
        slot = lax.rem(layer, SLOTS)
        grad = jnp.dot(a_v[layer], b_v[slot], preferred_element_type=jnp.float32)
        g_v[layer] = grad
        sq = grad * grad + EPS_ONE
        lane_part = jnp.sum(sq, axis=0, keepdims=True)
        part = sq[:, :LANES]
        for k in range(chunks):
            cols = slice(k * LANES, (k + 1) * LANES)
            if k:
                part = part + sq[:, cols]
            mine[k:k + 1, :] = lane_part[:, cols]
        pair_buf[layer, core, :2 * depth, :] = part

    def send_pair(layer):
        send(pair_buf.at[layer, core], pair_buf.at[layer, core], pair_sem.at[layer], dev(row, 1 - core), 2)

    def total(buf, count):
        out = buf[0]
        for s in range(1, count):
            out = out + buf[s]
        return out

    def wait_d(layer):
        arrived(w_v.at[:, layer], w_sem.at[layer])
        arrived(side_buf.at[layer, pl.ds(0, depth)], so_sem.at[layer])
        arrived(pair_buf.at[layer, 0], pair_sem.at[layer])

    def work_d(layer):
        d, role, mate = pair(layer)
        both = total(pair_buf.at[layer], 2)
        side_sum = jnp.sum(both[:2 * depth], axis=1, keepdims=True)
        new = beta * side_buf[layer] + side_sum * (keep / n_lane)
        side_buf[layer] = new
        inv = lax.rsqrt(new)
        axis = lax.rem(d + 1, 3)
        me = pos_of(axis)
        mine = p_buf.at[0, layer, me]
        for k in range(chunks):
            cols = slice(k * LANES, (k + 1) * LANES)
            upd = g_v[layer, :, cols] * inv
            g_v[layer, :, cols] = upd
            mine[half + k:half + k + 1, :] = jnp.sum(upd * upd, axis=0, keepdims=True)
        w_sum = []
        for j in range(2):
            w_sq = None
            for k in range(chunks):
                wgt = w_v[j, layer, :, k * LANES:(k + 1) * LANES]
                w_sq = wgt * wgt if k == 0 else w_sq + wgt * wgt
            w_sum.append(jnp.sum(jnp.sum(w_sq, axis=0, keepdims=True), axis=1, keepdims=True) * (2.0 / LANES))
        mine[2 * half - 1:2 * half, :] = jnp.where(left, w_sum[0], w_sum[1])
        mean_in = jnp.sum(new, axis=0, keepdims=True) * (1.0 / (n_side * LANES))
        mean_out = jnp.broadcast_to(jnp.sum(side_sum, axis=0, keepdims=True), (1, LANES)) * (keep / (n_total * LANES))
        mean_out = mean_out + both[2 * depth:2 * depth + 1] * (beta / (n_lane * (n_row // 2)))
        mine[chunks:half, :] = jnp.where(role == 0, mean_in, mean_out)

    def send_d(layer):
        d, role, mate = pair(layer)
        axis = lax.rem(d + 1, 3)
        me = pos_of(axis)
        mine = p_buf.at[0, layer, me]
        for t in range(1, side):
            send(mine, mine, p_sem.at[0, layer], dev(moved(axis, lax.rem(me + t, side)), core), 3)
        send(g_v.at[layer, pl.ds(depth, depth)], r_v.at[layer], g_sem.at[layer], dev(mate, core), 4)
        send(side_buf.at[layer, pl.ds(depth, depth)], side_back.at[layer], sb_sem.at[layer], dev(mate, core), 5)

    def stage_p(step, layer):
        arrived(p_buf.at[step, layer, pl.ds(0, side - 1)], p_sem.at[step, layer])
        axis = lax.rem(pair(layer)[0] + step + 2, 3)
        me = pos_of(axis)
        mine = p_buf.at[step + 1, layer, me]
        mine[...] = total(p_buf.at[step, layer], side)
        for t in range(1, side):
            send(mine, mine, p_sem.at[step + 1, layer], dev(moved(axis, lax.rem(me + t, side)), core), 6 + step)

    def stage_z(layer):
        arrived(p_buf.at[2, layer, pl.ds(0, side - 1)], p_sem.at[2, layer])
        weights = None
        for j in range(2):
            low = p_buf[2, layer, j, :half]
            high = p_buf[2, layer, j, half:]
            for s in range(j + 2, side, 2):
                low = low + p_buf[2, layer, s, :half]
                high = high + p_buf[2, layer, s, half:]
            new = jnp.where(real, beta * old_pack[layer, j] + low * (keep / n_side), 1.0)
            new_pack[layer, j] = new
            mean = jnp.sum(low[chunks:half], axis=1, keepdims=True)
            u = lax.rsqrt(new) * jnp.sqrt(mean)
            u_v[layer, j] = u
            fin_buf[layer, core, j:j + 1, :] = jnp.sum(jnp.where(real, (high * u) * u, 0.0), axis=0, keepdims=True)
            weights = high[half - 1:half] if j == 0 else weights + high[half - 1:half]
        fin_buf[layer, core, 2:3, :] = jnp.where(left, weights, 0.0)
        fin_buf[layer, core, 3:4, :] = jnp.where(left, 0.0, weights)
        fin_buf[layer, core, 4:, :] = jnp.zeros((4, LANES), jnp.float32)
        send(fin_buf.at[layer, core], fin_buf.at[layer, core], fin_sem.at[layer], dev(row, 1 - core), 8)

    def stage_f(layer):
        role = pair(layer)[1]
        arrived(r_v.at[layer], g_sem.at[layer])
        arrived(fin_buf.at[layer, 0], fin_sem.at[layer])
        rms = jnp.sqrt(jnp.sum(total(fin_buf.at[layer], 2), axis=1, keepdims=True) / n_total)
        amount = hyper_s[1] * jnp.maximum(EPS_TWO, rms[2:4]) / jnp.maximum(1.0, rms[0:2] / hyper_s[2])
        for j in range(2):
            fac_v[j] = u_v[layer, j] * amount[j:j + 1]
        for k in range(chunks):
            cols = slice(k * LANES, (k + 1) * LANES)
            w_v[role, layer, :, cols] = w_v[role, layer, :, cols] - g_v[layer, :depth, cols] * fac_v[role, k:k + 1, :]
            w_v[1 - role, layer, :, cols] = w_v[1 - role, layer, :, cols] - r_v[layer, :, cols] * fac_v[1 - role, k:k + 1, :]

    def at(i, lag, stage, count):
        pl.when((i >= lag) & (i < count + lag))(lambda: stage(i - lag))

    lag_z = LAG_D + 3 * LAG

    def exchange(i):
        at(i, LAG_D + LAG, functools.partial(stage_p, 0), layers)
        at(i, LAG_D + 2 * LAG, functools.partial(stage_p, 1), layers)
        at(i, lag_z, stage_z, layers)
        at(i, lag_z + 1, stage_f, layers - 1)

    def fill(i, carry):
        wait_a(i)
        work_a(i)
        send_pair(i)
        pl.when(i + SLOTS < layers)(lambda: b_start(i + SLOTS))
        return carry

    def steady(i, carry):
        wait_d(i - LAG_D)
        wait_a(i)
        work_d(i - LAG_D)
        work_a(i)
        send_pair(i)
        send_d(i - LAG_D)
        pl.when(i + SLOTS < layers)(lambda: b_start(i + SLOTS))
        exchange(i)
        return carry

    def drain(i, carry):
        @pl.when(i < layers + LAG_D)
        def _():
            wait_d(i - LAG_D)
            work_d(i - LAG_D)
            send_d(i - LAG_D)

        exchange(i)
        return carry

    lax.fori_loop(0, LAG_D, fill, 0)
    for layer in range(layers):
        for j in range(2):
            for k in range(chunks):
                old_pack[layer, j, k:k + 1, :] = lane_old[j, layer:layer + 1, k * LANES:(k + 1) * LANES]
            old_pack[layer, j, chunks:, :] = jnp.ones((half - chunks, LANES), jnp.float32)
    lax.fori_loop(LAG_D, layers, steady, 0)
    lax.fori_loop(layers, layers + lag_z, drain, 0)

    for layer in range(layers):
        role = pair(layer)[1]
        arrived(side_back.at[layer], sb_sem.at[layer])
        for j in range(2):
            for k in range(chunks):
                lane_res[j, layer:layer + 1, k * LANES:(k + 1) * LANES] = new_pack[layer, j, k:k + 1, :]
        side_res[role, layer:layer + 1, :] = jnp.sum(jnp.where(eye, side_buf[layer, :depth, :depth], 0.0), axis=0, keepdims=True)
        side_res[1 - role, layer:layer + 1, :] = jnp.sum(jnp.where(eye, side_back[layer, :, :depth], 0.0), axis=0, keepdims=True)
    stage_f(layers - 1)

    def sent(ref, k):
        pltpu.make_async_copy(ref, ref, send_sem.at[k]).wait()

    sent(a_v.at[:, pl.ds(0, depth)], 0)
    sent(side_out_buf, 1)
    sent(pair_buf.at[:, 0], 2)
    sent(p_buf.at[0, :, pl.ds(0, side - 1)], 3)
    sent(r_v, 4)
    sent(side_back, 5)
    sent(p_buf.at[1, :, pl.ds(0, side - 1)], 6)
    sent(p_buf.at[2, :, pl.ds(0, side - 1)], 7)
    sent(fin_buf.at[:, 0], 8)


def write_kernel(w_v, side_v, lane_v, o_w_in, o_side_in, o_lane_in, o_w_out, o_lane_out, o_side_out, sem):
    pairs = [(w_v.at[0], o_w_in), (w_v.at[1], o_w_out), (lane_v.at[0], o_lane_in), (lane_v.at[1], o_lane_out), (side_v.at[0], o_side_in), (side_v.at[1], o_side_out)]
    copies = [pltpu.make_async_copy(s, d, sem.at[i]) for i, (s, d) in enumerate(pairs)]
    for c in copies:
        c.start()
    for c in copies:
        c.wait()


def solution(mesh):
    side = torus_side(mesh.shape['row'])
    tile_in = P(None, 'row', 'col')
    tile_out = P(None, 'col', 'row')
    lane_row = P(None, None, 'row')
    lane_col = P(None, None, 'col')
    vec_row = P(None, 'row')
    vec_col = P(None, 'col')

    def local_step(hyper_params, w_in, x_in, dy_in, row_in, col_in, w_out, x_out, dy_out, row_out, col_out):
        layers, depth, width = w_in.shape
        tokens = x_in.shape[1]
        chunks = width // LANES
        half = chunks + 1
        f32 = jnp.float32
        turn = lambda v: jnp.swapaxes(v, 1, 2)
        vm = pltpu.VMEM
        dma = pltpu.SemaphoreType.DMA
        scratch = [
            pltpu.SMEM((3,), f32), vm((layers, 2 * depth, tokens), jnp.bfloat16), vm((layers, depth, tokens), jnp.bfloat16), vm((SLOTS, tokens, width), jnp.bfloat16),
            vm((layers, 2 * depth, width), f32), vm((layers, depth, width), f32),
            vm((2, layers, depth), f32), vm((2, layers, width), f32), vm((layers, 2, half, LANES), f32),
            vm((layers, 2 * depth, LANES), f32), vm((layers, depth, LANES), f32), vm((layers, depth, LANES), f32),
            vm((2, half, LANES), f32), vm((layers, 2, half, LANES), f32), vm((layers, 2, half, LANES), f32),
            vm((layers, 2, 2 * depth + 8, LANES), f32), vm((3, layers, side, 2 * half, LANES), f32), vm((layers, 2, 8, LANES), f32),
            dma((5,)), dma((layers,)), dma((layers,)), dma((layers,)), dma((layers,)), dma((SLOTS,)), dma((9,)), dma((layers,)), dma((layers,)), dma((layers,)), dma((3, layers)), dma((layers,)), dma((layers,)),
        ]
        in_vmem = pl.BlockSpec(memory_space=vm)
        anywhere = pl.BlockSpec(memory_space=pl.ANY)
        held = pl.pallas_call(
            functools.partial(kernel, side),
            out_shape=(vm((2, layers, depth, width), f32), vm((2, layers, depth), f32), vm((2, layers, width), f32)),
            in_specs=[pl.BlockSpec(memory_space=pltpu.HBM)] * 11,
            out_specs=[in_vmem] * 3,
            scratch_shapes=scratch,
            name="adafactor_step",
            compiler_params=pltpu.CompilerParams(collective_id=0, has_side_effects=True, vmem_limit_bytes=VMEM_LIMIT),
        )(*[pltpu.with_memory_space_constraint(v, pltpu.HBM) for v in (hyper_params, turn(x_in), dy_in, w_in, row_in, col_in, turn(dy_out), x_out, turn(w_out), row_out, col_out)])
        shape = lambda *s: jax.ShapeDtypeStruct(s, f32)
        res = pl.pallas_call(
            write_kernel,
            out_shape=(shape(layers, depth, width), shape(layers, depth), shape(layers, width), shape(layers, depth, width), shape(layers, width), shape(layers, depth)),
            in_specs=[anywhere] * 3,
            out_specs=[anywhere] * 6,
            scratch_shapes=[dma((6,))],
            name="write_back",
            compiler_params=pltpu.CompilerParams(vmem_limit_bytes=4 * 1024 * 1024),
        )(*held)
        return res[0], res[1], res[2], turn(res[3]), res[4], res[5]

    return jax.shard_map(local_step, mesh=mesh, in_specs=(P(), tile_in, lane_row, lane_col, vec_row, vec_col, tile_out, lane_col, lane_row, vec_col, vec_row), out_specs=(tile_in, vec_row, vec_col, tile_out, vec_col, vec_row), check_vma=False)
```

```python
import functools

import jax
import jax.numpy as jnp
from jax import lax
from jax.experimental import pallas as pl
from jax.experimental.pallas import tpu as pltpu
from jax.sharding import PartitionSpec as P

EPS_ONE = 1e-30
EPS_TWO = 1e-3
MESH = pl.DeviceIdType.MESH
LANES = 128
SLOTS = 6
LAG = 7
LAG_D = 4
EARLY = 6
VMEM_LIMIT = 48 * 1024 * 1024


def torus_side(n_row):
    return round(n_row ** (1.0 / 3.0))


def kernel(side, hyper, a_in, b_in, w_in, side_in, lane_in, a_out, b_out, w_out, lane_out, side_out,
           w_v, side_res, lane_res,
           hyper_s, a_v, ax_v, b_v, g_v, r_v, side_old, lane_old, old_pack, side_buf, side_out_buf, side_back,
           fac_v, new_pack, u_v, pair_buf, p_buf, fin_buf,
           load_sem, a_sem, ar_sem, ax_sem, w_sem, b_sem, send_sem, so_sem, sb_sem, pair_sem, p_sem, g_sem, fin_sem):
    layers, depth, width = w_in.shape
    chunks = width // LANES
    half = chunks + 1
    n_row = side ** 3
    n_side = float(depth * n_row)
    n_lane = float(width * 2)
    n_total = n_side * n_lane

    row = lax.axis_index("row")
    core = lax.axis_index("col")

    def stride_of(d):
        return 1 + (side - 1) * d + ((side - 1) * (side - 1) * d * (d - 1)) // 2

    def pos_of(d):
        return lax.rem(row // stride_of(d), side)

    def moved(d, pos):
        return row + (pos - pos_of(d)) * stride_of(d)

    def pair(layer):
        kind = lax.rem(layer, 6)
        d = kind // 2
        flavour = lax.rem(kind, 2)
        pos = pos_of(d)
        role = lax.rem(pos, 2)
        mate = lax.rem(pos + (1 - 2 * role) * (1 - 2 * flavour) + side, side)
        return d, role, moved(d, mate)

    def dev(r, c):
        return {"row": r, "col": c}

    b_refs = (b_in, b_out)
    a_refs = (a_in, a_out)
    w_refs = (w_in, w_out)

    def b_start(layer):
        slot = lax.rem(layer, SLOTS)
        role = pair(layer)[1]
        for j in range(2):
            @pl.when(role == j)
            def _():
                pltpu.make_async_copy(b_refs[j].at[layer], b_v.at[slot], b_sem.at[slot]).start()
            pltpu.make_async_copy(w_refs[j].at[layer], w_v.at[j, layer], w_sem.at[layer]).start()

    small = [(hyper, hyper_s), (side_in, side_old.at[0]), (side_out, side_old.at[1]), (lane_in, lane_old.at[0]), (lane_out, lane_old.at[1])]
    small = [pltpu.make_async_copy(s, d, load_sem.at[i]) for i, (s, d) in enumerate(small)]
    barrier = pltpu.get_barrier_semaphore()
    peers = [dev(moved(d, lax.rem(pos_of(d) + t, side)), core) for d in range(3) for t in range(1, side)] + [dev(row, 1 - core)]
    for d in peers:
        pl.semaphore_signal(barrier, inc=1, device_id=d, device_id_type=MESH)
    for c in small:
        c.start()

    def load_a(layer, carry):
        role = pair(layer)[1]
        for j in range(2):
            @pl.when(role == j)
            def _():
                pltpu.make_async_copy(a_refs[1 - j].at[layer], ax_v.at[layer], ax_sem.at[layer]).start()
                pltpu.make_async_copy(a_refs[j].at[layer], a_v.at[layer, pl.ds(0, depth)], a_sem.at[layer]).start()
        return carry

    lax.fori_loop(0, layers, load_a, 0)
    for s in range(SLOTS):
        b_start(s)

    def send(src, dst, recv, d, k):
        pltpu.make_async_remote_copy(src_ref=src, dst_ref=dst, send_sem=send_sem.at[k], recv_sem=recv, device_id=d, device_id_type=MESH).start()

    def arrived(ref, sem):
        pltpu.make_async_copy(ref, ref, sem).wait()

    def send_a(layer):
        arrived(ax_v.at[layer], ax_sem.at[layer])
        send(ax_v.at[layer], a_v.at[layer, pl.ds(depth, depth)], ar_sem.at[layer], dev(pair(layer)[2], core), 0)

    pl.semaphore_wait(barrier, len(peers))
    for layer in range(EARLY):
        send_a(layer)
    for c in small:
        c.wait()

    beta = hyper_s[0]
    keep = 1.0 - beta
    eye = lax.broadcasted_iota(jnp.int32, (depth, depth), 0) == lax.broadcasted_iota(jnp.int32, (depth, depth), 1)
    half_id = lax.broadcasted_iota(jnp.int32, (half, LANES), 0)
    real = half_id < chunks
    left = lax.broadcasted_iota(jnp.int32, (1, LANES), 1) < LANES // 2

    old_sum = lane_old[1, :, :LANES]
    for k in range(1, chunks):
        old_sum = old_sum + lane_old[1, :, k * LANES:(k + 1) * LANES]
    for layer in range(layers):
        role = pair(layer)[1]
        column = []
        for j in range(2):
            line = jnp.broadcast_to(side_old[j, layer:layer + 1, :], (depth, depth))
            line = jnp.sum(jnp.where(eye, line, 0.0), axis=1, keepdims=True)
            column.append(jnp.broadcast_to(line, (depth, LANES)))
        side_buf[layer, :depth, :] = jnp.where(role == 0, column[0], column[1])
        side_out_buf[layer] = jnp.where(role == 0, column[1], column[0])
        pair_buf[layer, core, 2 * depth:, :] = jnp.broadcast_to(old_sum[layer:layer + 1], (8, LANES))

    def send_side(layer, carry):
        mate = pair(layer)[2]
        send(side_out_buf.at[layer], side_buf.at[layer, pl.ds(depth, depth)], so_sem.at[layer], dev(mate, core), 1)
        pl.when(layer >= EARLY)(lambda: send_a(layer))
        return carry

    lax.fori_loop(0, layers, send_side, 0)

    def wait_a(layer):
        slot = lax.rem(layer, SLOTS)
        arrived(a_v.at[layer, pl.ds(0, depth)], a_sem.at[layer])
        arrived(a_v.at[layer, pl.ds(0, depth)], ar_sem.at[layer])
        arrived(b_v.at[slot], b_sem.at[slot])

    def work_a(layer):
        d, role, mate = pair(layer)
        mine = p_buf.at[0, layer, pos_of(lax.rem(d + 1, 3))]
        slot = lax.rem(layer, SLOTS)
        grad = jnp.dot(a_v[layer], b_v[slot], preferred_element_type=jnp.float32)
        g_v[layer] = grad
        sq = grad * grad + EPS_ONE
        lane_part = jnp.sum(sq, axis=0, keepdims=True)
        part = sq[:, :LANES]
        for k in range(chunks):
            cols = slice(k * LANES, (k + 1) * LANES)
            if k:
                part = part + sq[:, cols]
            mine[k:k + 1, :] = lane_part[:, cols]
        pair_buf[layer, core, :2 * depth, :] = part

    def send_pair(layer):
        send(pair_buf.at[layer, core], pair_buf.at[layer, core], pair_sem.at[layer], dev(row, 1 - core), 2)

    def total(buf, count):
        out = buf[0]
        for s in range(1, count):
            out = out + buf[s]
        return out

    def wait_d(layer):
        arrived(w_v.at[:, layer], w_sem.at[layer])
        arrived(side_buf.at[layer, pl.ds(0, depth)], so_sem.at[layer])
        arrived(pair_buf.at[layer, 0], pair_sem.at[layer])

    def work_d(layer):
        d, role, mate = pair(layer)
        both = total(pair_buf.at[layer], 2)
        side_sum = jnp.sum(both[:2 * depth], axis=1, keepdims=True)
        new = beta * side_buf[layer] + side_sum * (keep / n_lane)
        side_buf[layer] = new
        inv = lax.rsqrt(new)
        axis = lax.rem(d + 1, 3)
        me = pos_of(axis)
        mine = p_buf.at[0, layer, me]
        for k in range(chunks):
            cols = slice(k * LANES, (k + 1) * LANES)
            upd = g_v[layer, :, cols] * inv
            g_v[layer, :, cols] = upd
            mine[half + k:half + k + 1, :] = jnp.sum(upd * upd, axis=0, keepdims=True)
        w_sum = []
        for j in range(2):
            w_sq = None
            for k in range(chunks):
                wgt = w_v[j, layer, :, k * LANES:(k + 1) * LANES]
                w_sq = wgt * wgt if k == 0 else w_sq + wgt * wgt
            w_sum.append(jnp.sum(jnp.sum(w_sq, axis=0, keepdims=True), axis=1, keepdims=True) * (2.0 / LANES))
        mine[2 * half - 1:2 * half, :] = jnp.where(left, w_sum[0], w_sum[1])
        mean_in = jnp.sum(new, axis=0, keepdims=True) * (1.0 / (n_side * LANES))
        mean_out = jnp.broadcast_to(jnp.sum(side_sum, axis=0, keepdims=True), (1, LANES)) * (keep / (n_total * LANES))
        mean_out = mean_out + both[2 * depth:2 * depth + 1] * (beta / (n_lane * (n_row // 2)))
        mine[chunks:half, :] = jnp.where(role == 0, mean_in, mean_out)

    def send_d(layer):
        d, role, mate = pair(layer)
        axis = lax.rem(d + 1, 3)
        me = pos_of(axis)
        mine = p_buf.at[0, layer, me]
        for t in range(1, side):
            send(mine, mine, p_sem.at[0, layer], dev(moved(axis, lax.rem(me + t, side)), core), 3)
        send(g_v.at[layer, pl.ds(depth, depth)], r_v.at[layer], g_sem.at[layer], dev(mate, core), 4)
        send(side_buf.at[layer, pl.ds(depth, depth)], side_back.at[layer], sb_sem.at[layer], dev(mate, core), 5)

    def stage_p(step, layer):
        arrived(p_buf.at[step, layer, pl.ds(0, side - 1)], p_sem.at[step, layer])
        axis = lax.rem(pair(layer)[0] + step + 2, 3)
        me = pos_of(axis)
        mine = p_buf.at[step + 1, layer, me]
        mine[...] = total(p_buf.at[step, layer], side)
        for t in range(1, side):
            send(mine, mine, p_sem.at[step + 1, layer], dev(moved(axis, lax.rem(me + t, side)), core), 6 + step)

    def stage_z(layer):
        arrived(p_buf.at[2, layer, pl.ds(0, side - 1)], p_sem.at[2, layer])
        weights = None
        for j in range(2):
            low = p_buf[2, layer, j, :half]
            high = p_buf[2, layer, j, half:]
            for s in range(j + 2, side, 2):
                low = low + p_buf[2, layer, s, :half]
                high = high + p_buf[2, layer, s, half:]
            new = jnp.where(real, beta * old_pack[layer, j] + low * (keep / n_side), 1.0)
            new_pack[layer, j] = new
            mean = jnp.sum(low[chunks:half], axis=1, keepdims=True)
            u = lax.rsqrt(new) * jnp.sqrt(mean)
            u_v[layer, j] = u
            fin_buf[layer, core, j:j + 1, :] = jnp.sum(jnp.where(real, (high * u) * u, 0.0), axis=0, keepdims=True)
            weights = high[half - 1:half] if j == 0 else weights + high[half - 1:half]
        fin_buf[layer, core, 2:3, :] = jnp.where(left, weights, 0.0)
        fin_buf[layer, core, 3:4, :] = jnp.where(left, 0.0, weights)
        fin_buf[layer, core, 4:, :] = jnp.zeros((4, LANES), jnp.float32)
        send(fin_buf.at[layer, core], fin_buf.at[layer, core], fin_sem.at[layer], dev(row, 1 - core), 8)

    def stage_f(layer):
        role = pair(layer)[1]
        arrived(r_v.at[layer], g_sem.at[layer])
        arrived(fin_buf.at[layer, 0], fin_sem.at[layer])
        rms = jnp.sqrt(jnp.sum(total(fin_buf.at[layer], 2), axis=1, keepdims=True) / n_total)
        amount = hyper_s[1] * jnp.maximum(EPS_TWO, rms[2:4]) / jnp.maximum(1.0, rms[0:2] / hyper_s[2])
        for j in range(2):
            fac_v[j] = u_v[layer, j] * amount[j:j + 1]
        for k in range(chunks):
            cols = slice(k * LANES, (k + 1) * LANES)
            w_v[role, layer, :, cols] = w_v[role, layer, :, cols] - g_v[layer, :depth, cols] * fac_v[role, k:k + 1, :]
            w_v[1 - role, layer, :, cols] = w_v[1 - role, layer, :, cols] - r_v[layer, :, cols] * fac_v[1 - role, k:k + 1, :]

    def at(i, lag, stage, count):
        pl.when((i >= lag) & (i < count + lag))(lambda: stage(i - lag))

    lag_z = LAG_D + 3 * LAG

    def exchange(i):
        at(i, LAG_D + LAG, functools.partial(stage_p, 0), layers)
        at(i, LAG_D + 2 * LAG, functools.partial(stage_p, 1), layers)
        at(i, lag_z, stage_z, layers)
        at(i, lag_z + 1, stage_f, layers - 1)

    def fill(i, carry):
        wait_a(i)
        work_a(i)
        send_pair(i)
        pl.when(i + SLOTS < layers)(lambda: b_start(i + SLOTS))
        return carry

    def steady(i, carry):
        wait_d(i - LAG_D)
        wait_a(i)
        work_d(i - LAG_D)
        work_a(i)
        send_pair(i)
        send_d(i - LAG_D)
        pl.when(i + SLOTS < layers)(lambda: b_start(i + SLOTS))
        exchange(i)
        return carry

    def drain(i, carry):
        @pl.when(i < layers + LAG_D)
        def _():
            wait_d(i - LAG_D)
            work_d(i - LAG_D)
            send_d(i - LAG_D)

        exchange(i)
        return carry

    lax.fori_loop(0, LAG_D, fill, 0)
    for layer in range(layers):
        for j in range(2):
            for k in range(chunks):
                old_pack[layer, j, k:k + 1, :] = lane_old[j, layer:layer + 1, k * LANES:(k + 1) * LANES]
            old_pack[layer, j, chunks:, :] = jnp.ones((half - chunks, LANES), jnp.float32)
    lax.fori_loop(LAG_D, layers, steady, 0)
    lax.fori_loop(layers, layers + lag_z, drain, 0)

    for layer in range(layers):
        role = pair(layer)[1]
        arrived(side_back.at[layer], sb_sem.at[layer])
        for j in range(2):
            for k in range(chunks):
                lane_res[j, layer:layer + 1, k * LANES:(k + 1) * LANES] = new_pack[layer, j, k:k + 1, :]
        side_res[role, layer:layer + 1, :] = jnp.sum(jnp.where(eye, side_buf[layer, :depth, :depth], 0.0), axis=0, keepdims=True)
        side_res[1 - role, layer:layer + 1, :] = jnp.sum(jnp.where(eye, side_back[layer, :, :depth], 0.0), axis=0, keepdims=True)
    stage_f(layers - 1)

    def sent(ref, k):
        pltpu.make_async_copy(ref, ref, send_sem.at[k]).wait()

    sent(a_v.at[:, pl.ds(0, depth)], 0)
    sent(side_out_buf, 1)
    sent(pair_buf.at[:, 0], 2)
    sent(p_buf.at[0, :, pl.ds(0, side - 1)], 3)
    sent(r_v, 4)
    sent(side_back, 5)
    sent(p_buf.at[1, :, pl.ds(0, side - 1)], 6)
    sent(p_buf.at[2, :, pl.ds(0, side - 1)], 7)
    sent(fin_buf.at[:, 0], 8)


def write_kernel(w_v, side_v, lane_v, o_w_in, o_side_in, o_lane_in, o_w_out, o_lane_out, o_side_out, sem):
    pairs = [(w_v.at[0], o_w_in), (w_v.at[1], o_w_out), (lane_v.at[0], o_lane_in), (lane_v.at[1], o_lane_out), (side_v.at[0], o_side_in), (side_v.at[1], o_side_out)]
    copies = [pltpu.make_async_copy(s, d, sem.at[i]) for i, (s, d) in enumerate(pairs)]
    for c in copies:
        c.start()
    for c in copies:
        c.wait()


def solution(mesh):
    side = torus_side(mesh.shape['row'])
    tile_in = P(None, 'row', 'col')
    tile_out = P(None, 'col', 'row')
    lane_row = P(None, None, 'row')
    lane_col = P(None, None, 'col')
    vec_row = P(None, 'row')
    vec_col = P(None, 'col')

    def local_step(hyper_params, w_in, x_in, dy_in, row_in, col_in, w_out, x_out, dy_out, row_out, col_out):
        layers, depth, width = w_in.shape
        tokens = x_in.shape[1]
        chunks = width // LANES
        half = chunks + 1
        f32 = jnp.float32
        turn = lambda v: jnp.swapaxes(v, 1, 2)
        vm = pltpu.VMEM
        dma = pltpu.SemaphoreType.DMA
        scratch = [
            pltpu.SMEM((3,), f32), vm((layers, 2 * depth, tokens), jnp.bfloat16), vm((layers, depth, tokens), jnp.bfloat16), vm((SLOTS, tokens, width), jnp.bfloat16),
            vm((layers, 2 * depth, width), f32), vm((layers, depth, width), f32),
            vm((2, layers, depth), f32), vm((2, layers, width), f32), vm((layers, 2, half, LANES), f32),
            vm((layers, 2 * depth, LANES), f32), vm((layers, depth, LANES), f32), vm((layers, depth, LANES), f32),
            vm((2, half, LANES), f32), vm((layers, 2, half, LANES), f32), vm((layers, 2, half, LANES), f32),
            vm((layers, 2, 2 * depth + 8, LANES), f32), vm((3, layers, side, 2 * half, LANES), f32), vm((layers, 2, 8, LANES), f32),
            dma((5,)), dma((layers,)), dma((layers,)), dma((layers,)), dma((layers,)), dma((SLOTS,)), dma((9,)), dma((layers,)), dma((layers,)), dma((layers,)), dma((3, layers)), dma((layers,)), dma((layers,)),
        ]
        in_vmem = pl.BlockSpec(memory_space=vm)
        anywhere = pl.BlockSpec(memory_space=pl.ANY)
        held = pl.pallas_call(
            functools.partial(kernel, side),
            out_shape=(vm((2, layers, depth, width), f32), vm((2, layers, depth), f32), vm((2, layers, width), f32)),
            in_specs=[pl.BlockSpec(memory_space=pltpu.HBM)] * 11,
            out_specs=[in_vmem] * 3,
            scratch_shapes=scratch,
            name="adafactor_step",
            compiler_params=pltpu.CompilerParams(collective_id=0, has_side_effects=True, vmem_limit_bytes=VMEM_LIMIT),
        )(*[pltpu.with_memory_space_constraint(v, pltpu.HBM) for v in (hyper_params, turn(x_in), dy_in, w_in, row_in, col_in, turn(dy_out), x_out, turn(w_out), row_out, col_out)])
        shape = lambda *s: jax.ShapeDtypeStruct(s, f32)
        res = pl.pallas_call(
            write_kernel,
            out_shape=(shape(layers, depth, width), shape(layers, depth), shape(layers, width), shape(layers, depth, width), shape(layers, width), shape(layers, depth)),
            in_specs=[anywhere] * 3,
            out_specs=[anywhere] * 6,
            scratch_shapes=[dma((6,))],
            name="write_back",
            compiler_params=pltpu.CompilerParams(vmem_limit_bytes=4 * 1024 * 1024),
        )(*held)
        return res[0], res[1], res[2], turn(res[3]), res[4], res[5]

    return jax.shard_map(local_step, mesh=mesh, in_specs=(P(), tile_in, lane_row, lane_col, vec_row, vec_col, tile_out, lane_col, lane_row, vec_col, vec_row), out_specs=(tile_in, vec_row, vec_col, tile_out, vec_col, vec_row), check_vma=False)
```
